512 devices in a mesh: seq: 128 (over z_lo, y, x), tp: 4 (over z_hi, core).
Axes of the slice: x: 4, y: 4, z: 16 (z_hi: 2, z_lo: 8; z = z_hi * 8 + z_lo), core: 2. Of those that a mesh axis runs over, the one named last changes fastest.
Arguments:
- inputs: bfloat16 [32768, 5120], P('seq', 'tp'), may hold values from -6 to 6
- gate_input: bfloat16 [32768, 5120], P('seq', 'tp'), may hold values from -6 to 6
- b_source: bfloat16 [32768, 128], P('seq'), may hold values from -6 to 6
- c_source: bfloat16 [32768, 128], P('seq'), may hold values from -6 to 6
- step_raw: float32 [32768, 80], P('seq', 'tp'), may hold values from -4 to 4
- step_bias: float32 [80], P('tp'), may hold values from -3 to 0
- decay_rate: float32 [80], P('tp'), may hold values from 6.1035157e-06 to 0.05
- conv_weight: float32 [4, 256], replicated, may hold values from -3 to 3
- conv_bias: float32 [256], replicated, may hold values from -3 to 3
- norm_gain: float32 [5120], P('tp'), may hold values from 0.5 to 1.5
- doc_lengths: int32 [8], replicated, may hold values from 1 to 16384, 32768 in all
Outputs:
- output: bfloat16 [32768, 5120], P('seq', 'tp')
The draws below stay inside these ranges and needn't reach their ends.
Inputs may be any that keep to these rules, and one draw needn't show every extreme that they name: doc_lengths sums to 32768; every length is at least 1 and the largest is exactly 16384.
All inputs are finite; a program needn't handle non-finite values.
Results may differ from the reference program's by a relative error of at most 0.0015.
Values may be sent and summed in bfloat16 or wider, within the bound.
A program may use at most 192 MiB of HBM per device.

```python
import math
import jax
import jax.numpy as jnp
import numpy as np
from jax import lax

H = 80
HEAD_DIM = 64
STATE = 128
CONV = 4
BLOCK = 256
DOCS = 8
SEQ = 32768
DOC_MOST = 16384


def steps_of(key, dims, shards, low, top_value):
    factor_of = 1.0
    for dim, shards_of in shards:
        steps = jax.random.uniform(jax.random.fold_in(jax.random.fold_in(key, 6), dim), (shards_of,), jnp.float32, low / len(shards), top_value / len(shards))
        factor_of = factor_of * jnp.repeat(jnp.exp(steps), dims[dim] // shards_of).reshape((-1,) + (1,) * (len(dims) - 1 - dim))
    return factor_of


def profile(number_of, total, bound, skew):
    loads = [(1 << 20) // math.isqrt(grade ** skew) + 1 for grade in range(2, number_of + 1)]
    surplus, holding = total - bound - (number_of - 1), [1] * (number_of - 1)
    while surplus > 0:
        candidates = [i for i in range(number_of - 1) if holding[i] < bound]
        pool, left = sum([loads[i] for i in candidates]), surplus
        for i in candidates:
            more = min(bound - holding[i], max(1, left * loads[i] // pool), surplus)
            holding[i] = holding[i] + more
            surplus = surplus - more
    return np.array([bound] + holding)


def ragged_sizes(rng, number_of, total, most, slope):
    if number_of == 2:
        one = jax.random.randint(rng, (), max(1, total - most), min(most, total - 1) + 1)
        return jnp.stack([one, total - one])
    lengths = jnp.asarray(profile(number_of, total, most, slope), jnp.int32)
    couples = (number_of - 1) // 2
    giver, sink = lengths[1:1 + 2 * couples:2], lengths[2:2 + 2 * couples:2]
    slack = jnp.minimum(giver - 1, most - sink)
    passed = jax.random.randint(jax.random.fold_in(rng, 1), (couples,), 0, 1 << 20) % (slack + 1)
    lengths = lengths.at[1:1 + 2 * couples:2].set(giver - passed).at[2:2 + 2 * couples:2].set(sink + passed)
    return lengths[jax.random.permutation(jax.random.fold_in(rng, 2), number_of)]


def normal_values(stream_key, extent, spread, reach, cuts=(), held_as=jnp.bfloat16):
    drawn = spread * jax.random.normal(stream_key, extent, jnp.float32)
    if cuts:
        drawn = drawn * steps_of(stream_key, extent, cuts, -0.22, 0.18)
    return jnp.clip(drawn, -reach, reach).astype(held_as)


def setup_inputs(seed: int = 0) -> dict:
    key_of = jax.random.split(jax.random.key(seed), 12)
    inputs = normal_values(key_of[0], (SEQ, H * HEAD_DIM), 1.0, 6.0, ((0, 128), (1, 4)))
    gate_input = normal_values(key_of[1], (SEQ, H * HEAD_DIM), 1.0, 6.0, ((0, 128), (1, 4)))
    b_source = normal_values(key_of[2], (SEQ, STATE), 1.0, 6.0, ((0, 128),))
    c_source = normal_values(key_of[3], (SEQ, STATE), 1.0, 6.0, ((0, 128),))
    step_raw = normal_values(key_of[4], (SEQ, H), 0.5, 4.0, ((0, 128), (1, 4)), jnp.float32)
    step_bias = jnp.clip(-3.0 + 3.0 * jax.random.uniform(key_of[5], (H,), jnp.float32) ** steps_of(key_of[5], (H,), ((0, 4),), -0.2, 0.2), -3.0, 0.0)
    decay_rate = jnp.clip(jnp.exp(math.log(0.05) - 9.010913 * jax.random.uniform(key_of[6], (H,), jnp.float32) ** steps_of(key_of[6], (H,), ((0, 4),), -0.2, 0.2)), 6.10351571594947e-06, 0.05)
    conv_weight = normal_values(key_of[7], (CONV, 2 * STATE), CONV ** -0.5, 3.0, (), jnp.float32)
    conv_bias = normal_values(key_of[8], (2 * STATE,), 0.5, 3.0, (), jnp.float32)
    norm_gain = jnp.clip(1.0 + 0.1 * jax.random.normal(key_of[9], (H * HEAD_DIM,), jnp.float32), 0.5, 1.5)
    doc_lengths = ragged_sizes(key_of[10], DOCS, SEQ, DOC_MOST, 2).astype(jnp.int32)
    return {"inputs": inputs, "gate_input": gate_input, "b_source": b_source, "c_source": c_source, "step_raw": step_raw, "step_bias": step_bias, "decay_rate": decay_rate, "conv_weight": conv_weight, "conv_bias": conv_bias, "norm_gain": norm_gain, "doc_lengths": doc_lengths}


epsilon = 1e-05

def locate(position, doc_lengths):
    starts = (jnp.cumsum(doc_lengths) - doc_lengths).astype(jnp.int32)
    chosen = jnp.where(starts[None, :] <= position[:, None], starts[None, :], 0)
    return lax.optimization_barrier(jnp.max(chosen, axis=1)).astype(jnp.int32)

def convolve(padded, weight, conv_bias, position, doc_start):
    kernel_taps = weight.shape[0]
    tokens = position.shape[0]
    widened = padded.astype(jnp.float32)
    summed = jnp.broadcast_to(conv_bias[None, :], (tokens, conv_bias.shape[0]))
    for offset in range(kernel_taps):
        backward = kernel_taps - 1 - offset
        inside = (position - backward >= doc_start)[:, None]
        summed = summed + jnp.where(inside, weight[offset][None, :] * widened[offset:offset + tokens], 0.0)
    return jax.nn.silu(summed).astype(jnp.bfloat16)

def state_terms(pieces):
    block_inputs, b_block, step_size, cumulated, doc_start, position = pieces
    same_doc = doc_start == doc_start[-1]
    weighting = jnp.where(same_doc[:, None], jnp.exp(cumulated[-1][None, :] - cumulated) * step_size, 0.0)
    weighted = (block_inputs.astype(jnp.float32) * weighting[:, :, None]).astype(jnp.bfloat16)
    weighted = lax.optimization_barrier(weighted).astype(jnp.float32)
    end_state = jnp.einsum('qhp,qn->hpn', weighted, b_block.astype(jnp.float32), precision=lax.Precision.HIGHEST)
    end_factor = jnp.where(doc_start[-1] < position[0], jnp.exp(cumulated[-1]), 0.0)
    return (end_state, end_factor)

def diagonal_terms(pieces):
    block_inputs, b_block, c_block, step_size, cumulated, doc_start = pieces
    row_count = doc_start.shape[0]
    products = jnp.dot(c_block, b_block.T, preferred_element_type=jnp.float32)
    order_ids = jnp.arange(row_count)
    causal = (order_ids[None, :] <= order_ids[:, None]) & (doc_start[None, :] == doc_start[:, None])
    decay_gap = cumulated.T[:, :, None] - cumulated.T[:, None, :]
    scores = jnp.where(causal[None], products[None] * jnp.exp(decay_gap) * step_size.T[:, None, :], 0.0)
    scores = lax.optimization_barrier(scores.astype(jnp.bfloat16)).astype(jnp.float32)
    return jnp.einsum('hts,shp->thp', scores, block_inputs.astype(jnp.float32), precision=lax.Precision.HIGHEST)

def emit_rows(state_in, pieces):
    end_state, end_factor, c_block, out_decay = pieces
    rounded = lax.optimization_barrier(state_in.astype(jnp.bfloat16)).astype(jnp.float32)
    from_state = jnp.einsum('qn,hpn->qhp', c_block.astype(jnp.float32), rounded, precision=lax.Precision.HIGHEST)
    from_state = from_state * out_decay[:, :, None]
    return (end_factor[:, None, None] * state_in + end_state, from_state)

def reference(inputs, gate_input, b_source, c_source, step_raw, step_bias, decay_rate, conv_weight, conv_bias, norm_gain, doc_lengths):
    position = jnp.arange(SEQ, dtype=jnp.int32)
    doc_start = locate(position, doc_lengths)
    keep_rows = CONV - 1
    blank = jnp.zeros((keep_rows, STATE), jnp.bfloat16)
    b_conv = convolve(jnp.concatenate([blank, b_source], 0), conv_weight[:, :STATE], conv_bias[:STATE], position, doc_start)
    c_conv = convolve(jnp.concatenate([blank, c_source], 0), conv_weight[:, STATE:], conv_bias[STATE:], position, doc_start)
    step_size = jax.nn.softplus(step_raw + step_bias[None, :])
    log_decay = -step_size * decay_rate[None, :]
    block_count = SEQ // BLOCK
    shaped_inputs = inputs.reshape(block_count, BLOCK, H, HEAD_DIM)
    b_blocks = b_conv.reshape(block_count, BLOCK, STATE)
    c_blocks = c_conv.reshape(block_count, BLOCK, STATE)
    step_blocks = step_size.reshape(block_count, BLOCK, H)
    cumulated = jnp.cumsum(log_decay.reshape(block_count, BLOCK, H), axis=1)
    start_blocks = doc_start.reshape(block_count, BLOCK)
    position_blocks = position.reshape(block_count, BLOCK)
    out_decay = jnp.where((start_blocks < position_blocks[:, :1])[:, :, None], jnp.exp(cumulated), 0.0)

    def advance(state_in, pieces):
        block_inputs, b_block, c_block, step_block, cum_block, start_block, position_block, decay_block = pieces
        end_state, end_factor = state_terms((block_inputs, b_block, step_block, cum_block, start_block, position_block))
        diagonal = diagonal_terms((block_inputs, b_block, c_block, step_block, cum_block, start_block))
        next_state, from_state = emit_rows(state_in, (end_state, end_factor, c_block, decay_block))
        return (next_state, diagonal + from_state)
    initial = jnp.zeros((H, HEAD_DIM, STATE), jnp.float32)
    final_state, mixed = lax.scan(advance, initial, (shaped_inputs, b_blocks, c_blocks, step_blocks, cumulated, start_blocks, position_blocks, out_decay))
    mixed = mixed.reshape(SEQ, H * HEAD_DIM)
    gated = mixed * jax.nn.silu(gate_input.astype(jnp.float32))
    mean_square = lax.optimization_barrier(jnp.sum(gated * gated, axis=1)) / (H * HEAD_DIM)
    return (gated * lax.rsqrt(mean_square + epsilon)[:, None] * norm_gain[None, :]).astype(jnp.bfloat16)
```

```python
import functools

import jax
import jax.numpy as jnp
from jax import lax
from jax.experimental import pallas as pl
from jax.experimental.pallas import tpu as pltpu
from jax.sharding import PartitionSpec as P

MESH = pl.DeviceIdType.MESH
EPS = 1e-05
SUPER = 32
HALVES = 2


def locate(position, doc_lengths):
    starts = (jnp.cumsum(doc_lengths) - doc_lengths).astype(jnp.int32)
    chosen = jnp.where(starts[None, :] <= position[:, None], starts[None, :], 0)
    return jnp.max(chosen, axis=1).astype(jnp.int32)


def convolve(padded, weight, conv_bias, position, doc_start):
    taps = weight.shape[0]
    tokens = position.shape[0]
    widened = padded.astype(jnp.float32)
    summed = jnp.broadcast_to(conv_bias[None, :], (tokens, conv_bias.shape[0]))
    for offset in range(taps):
        inside = (position - (taps - 1 - offset) >= doc_start)[:, None]
        summed = summed + jnp.where(
            inside, weight[offset][None, :] * widened[offset : offset + tokens], 0.0
        )
    return jax.nn.silu(summed).astype(jnp.bfloat16)


def carry_kernel(
    groups, e_ref, f_ref, q_ref, er, fr, tot, ztot, qs, qr, wide, fs, zfs,
    e_send, e_recv, f_send, f_recv, z_send, z_recv, zf_send, zf_recv, q_send, q_recv,
):
    me = lax.axis_index("seq")
    group, place = me // SUPER, me % SUPER
    dz, dy, dx = place // 16, (place // 4) % 4, place % 4
    rows, lanes = er.shape[1], er.shape[2]

    def partner(d):
        to = ((dz + d // 16) % 2) * 16 + ((dy + (d // 4) % 4) % 4) * 4 + (dx + d % 4) % 4
        return to, group * SUPER + to

    barrier = pltpu.get_barrier_semaphore()

    def greet(d, carry):
        pl.semaphore_signal(barrier, 1, device_id={"seq": partner(d)[1]}, device_id_type=MESH)
        return carry

    lax.fori_loop(1, SUPER, greet, 0)
    for k in range(1, groups):
        there = ((group + k) % groups) * SUPER + place
        pl.semaphore_signal(barrier, 1, device_id={"seq": there}, device_id_type=MESH)
    pl.semaphore_wait(barrier, SUPER - 1 + groups - 1)

    def f_copy(d):
        return pltpu.make_async_remote_copy(
            f_ref, fr.at[place], f_send.at[d], f_recv.at[d],
            device_id={"seq": partner(d)[1]}, device_id_type=MESH,
        )

    def e_copy(d):
        to = partner(d)[0]
        source = e_ref.at[
            pl.ds(pl.multiple_of((to // HALVES) * rows, 8), rows),
            pl.ds(pl.multiple_of((to % HALVES) * lanes, 128), lanes),
        ]
        return pltpu.make_async_remote_copy(
            source, er.at[place], e_send.at[d], e_recv.at[d],
            device_id={"seq": partner(d)[1]}, device_id_type=MESH,
        )

    def q_copy(d):
        to, there = partner(d)
        return pltpu.make_async_remote_copy(
            qs.at[to], qr.at[place], q_send.at[d], q_recv.at[d],
            device_id={"seq": there}, device_id_type=MESH,
        )

    def start_e(d, carry):
        f_copy(d).start()
        e_copy(d).start()
        return carry

    lax.fori_loop(1, SUPER, start_e, 0)
    fr[place] = f_ref[...]
    er[place] = e_ref[
        pl.ds(pl.multiple_of((place // HALVES) * rows, 8), rows),
        pl.ds(pl.multiple_of((place % HALVES) * lanes, 128), lanes),
    ]

    def wait_e(d, carry):
        f_copy(d).wait()
        e_copy(d).wait()
        return carry

    lax.fori_loop(1, SUPER, wait_e, 0)

    heads = f_ref.shape[1]
    width = lanes // 10
    column = lax.broadcasted_iota(jnp.int32, (heads, lanes), 1) // width + (place % HALVES) * 10
    pick = (column == lax.broadcasted_iota(jnp.int32, (heads, lanes), 0)).astype(jnp.float32)

    def expand(row):
        return jnp.dot(
            jnp.broadcast_to(row, (8, heads)), pick,
            precision=lax.Precision.HIGHEST, preferred_element_type=jnp.float32,
        )

    def spread(k, carry):
        fs[k] = expand(fr[k])
        return carry

    lax.fori_loop(0, SUPER, spread, 0)

    def total(k, pair):
        state, factor = pair
        return fs[k] * state + er[k], fr[k] * factor

    state, factor = lax.fori_loop(
        0, SUPER, total, (jnp.zeros((rows, lanes), jnp.float32), jnp.ones((1, heads), jnp.float32))
    )
    tot[...] = state
    zfs[...] = factor

    def z_copies(k):
        there = (group + k) * SUPER + place
        device = {"seq": there}
        return (
            pltpu.make_async_remote_copy(
                tot, ztot.at[pl.ds(group, 1)].at[0], z_send.at[k], z_recv.at[k],
                device_id=device, device_id_type=MESH,
            ),
            pltpu.make_async_remote_copy(
                zfs, wide.at[pl.ds(group, 1)].at[0], zf_send.at[k], zf_recv.at[k],
                device_id=device, device_id_type=MESH,
            ),
        )

    for k in range(1, groups):
        @pl.when(group + k < groups)
        def _():
            for copy in z_copies(k):
                copy.start()

    for k in range(1, groups):
        @pl.when(group - k >= 0)
        def _():
            for copy in z_copies(k):
                copy.wait_recv()

    er_in = jnp.zeros((rows, lanes), jnp.float32)
    for k in range(groups - 1):
        er_in = jnp.where(k < group, expand(wide[k]) * er_in + ztot[k], er_in)

    def emit(k, state):
        qs[k] = state.astype(jnp.bfloat16)
        return fs[k] * state + er[k]

    lax.fori_loop(0, SUPER, emit, er_in)

    def start_q(d, carry):
        q_copy(d).start()
        return carry

    lax.fori_loop(1, SUPER, start_q, 0)
    qr[place] = qs[place]

    for k in range(1, groups):
        @pl.when(group + k < groups)
        def _():
            for copy in z_copies(k):
                copy.wait_send()

    def wait_q(d, carry):
        q_copy(d).wait()
        return carry

    lax.fori_loop(1, SUPER, wait_q, 0)
    for k in range(0, SUPER // HALVES, 2):
        for half in range(HALVES):
            pair = [qr[(k + u) * HALVES + half].astype(jnp.float32) for u in range(2)]
            q_ref[k * rows : (k + 2) * rows, half * lanes : (half + 1) * lanes] = jnp.concatenate(
                pair, 0
            ).astype(jnp.bfloat16)


def carried(ends, factor, groups):
    state, features = ends.shape
    rows, lanes = state * HALVES // SUPER, features // HALVES
    f32 = jnp.float32
    dma = pltpu.SemaphoreType.DMA
    return pl.pallas_call(
        functools.partial(carry_kernel, groups),
        out_shape=jax.ShapeDtypeStruct((state, features), jnp.bfloat16),
        in_specs=[pl.BlockSpec(memory_space=pltpu.VMEM)] * 2,
        out_specs=pl.BlockSpec(memory_space=pltpu.VMEM),
        scratch_shapes=[
            pltpu.VMEM((SUPER, rows, lanes), f32),
            pltpu.VMEM((SUPER, 1, 128), f32),
            pltpu.VMEM((rows, lanes), f32),
            pltpu.VMEM((groups, rows, lanes), f32),
            pltpu.VMEM((SUPER, rows, lanes), jnp.bfloat16),
            pltpu.VMEM((SUPER, rows, lanes), jnp.bfloat16),
            pltpu.VMEM((groups, 1, 128), f32),
            pltpu.VMEM((SUPER, rows, lanes), f32),
            pltpu.VMEM((1, 128), f32),
            dma((SUPER,)), dma((SUPER,)), dma((SUPER,)), dma((SUPER,)),
            dma((groups,)), dma((groups,)), dma((groups,)), dma((groups,)),
            dma((SUPER,)), dma((SUPER,)),
        ],
        compiler_params=pltpu.CompilerParams(collective_id=0, has_side_effects=True),
    )(ends, factor)


def square_kernel(count, s_ref, o_ref, parts, send, recv):
    me = lax.axis_index("tp")
    barrier = pltpu.get_barrier_semaphore()
    for k in range(1, count):
        pl.semaphore_signal(
            barrier, 1, device_id={"tp": (me + k) % count}, device_id_type=MESH
        )
    pl.semaphore_wait(barrier, count - 1)
    copies = [
        pltpu.make_async_remote_copy(
            s_ref, parts.at[k - 1], send.at[k - 1], recv.at[k - 1],
            device_id={"tp": (me + k) % count}, device_id_type=MESH,
        )
        for k in range(1, count)
    ]
    for copy in copies:
        copy.start()
    for copy in copies:
        copy.wait()
    mine = [parts[k] for k in range(count - 1)]
    o_ref[...] = s_ref[...] + (mine[0] + mine[1] + mine[2])


def row_totals(sums, count):
    dma = pltpu.SemaphoreType.DMA
    shape = sums.shape
    return pl.pallas_call(
        functools.partial(square_kernel, count),
        out_shape=jax.ShapeDtypeStruct(shape, jnp.float32),
        in_specs=[pl.BlockSpec(memory_space=pltpu.VMEM)],
        out_specs=pl.BlockSpec(memory_space=pltpu.VMEM),
        scratch_shapes=[
            pltpu.VMEM((count - 1,) + shape, jnp.float32), dma((count - 1,)), dma((count - 1,)),
        ],
        compiler_params=pltpu.CompilerParams(collective_id=1, has_side_effects=True),
    )(sums)


def body(
    inputs, gate_input, b_source, c_source, step_raw, step_bias, decay_rate,
    conv_weight, conv_bias, norm_gain, doc_lengths,
):
    shards, parts = lax.axis_size("seq"), lax.axis_size("tp")
    tokens = inputs.shape[0]
    heads = step_raw.shape[1]
    width = inputs.shape[1] // heads
    state = b_source.shape[1]
    keep = conv_weight.shape[0] - 1
    f32 = jnp.float32
    position = lax.axis_index("seq") * tokens + jnp.arange(tokens, dtype=jnp.int32)
    doc_start = locate(position, doc_lengths)
    source = jnp.concatenate([b_source, c_source], 1)
    before = lax.ppermute(
        source[tokens - keep :], "seq", [(k, k + 1) for k in range(shards - 1)]
    )
    conv = convolve(
        jnp.concatenate([before, source], 0), conv_weight, conv_bias, position, doc_start
    )
    b_conv, c_conv = conv[:, :state], conv[:, state:]
    step = jax.nn.softplus(step_raw + step_bias[None, :])
    cumulated = jnp.cumsum(-step * decay_rate[None, :], axis=0)
    same = (doc_start == doc_start[-1])[:, None]
    weighting = jnp.where(same, jnp.exp(cumulated[-1][None, :] - cumulated) * step, 0.0)
    weighted = (
        inputs.reshape(tokens, heads, width).astype(f32) * weighting[:, :, None]
    ).astype(jnp.bfloat16).reshape(tokens, heads * width)
    ends = lax.dot_general(
        b_conv, weighted, (((0,), (0,)), ((), ())), preferred_element_type=f32
    )
    factor = jnp.where(doc_start[-1] < position[0], jnp.exp(cumulated[-1]), 0.0)
    factor = jnp.concatenate([factor, jnp.zeros((128 - heads,), f32)])[None, :]
    q = carried(ends, factor, shards // SUPER)

    products = jnp.dot(c_conv, b_conv.T, preferred_element_type=f32)
    order = jnp.arange(tokens)
    causal = (order[None, :] <= order[:, None]) & (doc_start[None, :] == doc_start[:, None])
    gap = cumulated.T[:, :, None] - cumulated.T[:, None, :]
    scores = jnp.where(causal[None], products[None] * jnp.exp(gap) * step.T[:, None, :], 0.0)
    diagonal = jnp.einsum(
        "hts,shp->thp", scores.astype(jnp.bfloat16), inputs.reshape(tokens, heads, width),
        preferred_element_type=f32,
    )
    out_decay = jnp.where((doc_start < position[0])[:, None], jnp.exp(cumulated), 0.0)
    from_state = jnp.dot(c_conv, q, preferred_element_type=f32).reshape(tokens, heads, width)
    mixed = (diagonal + from_state * out_decay[:, :, None]).reshape(tokens, heads * width)
    gated = mixed * jax.nn.silu(gate_input.astype(f32))
    sums = jnp.sum(gated * gated, axis=1).reshape(tokens // 128, 128)
    mean_square = row_totals(sums, parts).reshape(tokens) / (heads * width * parts)
    return (gated * lax.rsqrt(mean_square + EPS)[:, None] * norm_gain[None, :]).astype(
        jnp.bfloat16
    )


def solution(mesh):
    both, seq = P("seq", "tp"), P("seq", None)
    return jax.shard_map(
        body, mesh=mesh,
        in_specs=(both, both, seq, seq, both, P("tp"), P("tp"), P(), P(), P("tp"), P()),
        out_specs=both, check_vma=False,
    )
```

```python
import functools

import jax
import jax.numpy as jnp
from jax import lax
from jax.experimental import pallas as pl
from jax.experimental.pallas import tpu as pltpu
from jax.sharding import PartitionSpec as P

MESH = pl.DeviceIdType.MESH
EPS = 1e-05
SUPER = 32
F32 = jnp.float32
BF16 = jnp.bfloat16
EXACT = lax.Precision.HIGHEST


def remote(source, target, send, recv, **device):
    return pltpu.make_async_remote_copy(
        source, target, send, recv, device_id=device, device_id_type=MESH
    )


def layer_kernel(
    groups, parts, heads,
    x_hbm, gate_hbm, b_ref, c_ref, step_ref, bias_ref, rate_ref, taps_ref, shift_ref, gain_ref,
    docs_ref, out_ref,
    x, gate, steps, ext, halo, weighted, c_conv, rows_c, factor, ends, er, fr, wide,
    carry_in, carry_out, qs, qr, q, dg, rs, sums, others,
    x_sem, h_send, h_recv, f_send, f_recv, e_send, e_recv, z_send, z_recv, q_send, q_recv,
    s_send, s_recv,
):
    me, part = lax.axis_index("seq"), lax.axis_index("tp")
    shards = groups * SUPER
    group, place = me // SUPER, me % SUPER
    dz, dy, dx = place // 16, (place // 4) % 4, place % 4
    tokens, features = x.shape
    state = b_ref.shape[1]
    rows, lanes = er.shape[1], er.shape[2]
    width = features // heads
    pairs = features // 128

    def partner(d):
        to = ((dz + d // 16) % 2) * 16 + ((dy + (d // 4) % 4) % 4) * 4 + (dx + d % 4) % 4
        return to, group * SUPER + to

    def each(f):
        def step(d, carry):
            f(d)
            return carry

        lax.fori_loop(1, SUPER, step, 0)

    x_in = pltpu.make_async_copy(x_hbm, x, x_sem.at[0])
    gate_in = pltpu.make_async_copy(gate_hbm, gate, x_sem.at[1])
    x_in.start()
    gate_in.start()

    barrier = pltpu.get_barrier_semaphore()

    def signal(**device):
        pl.semaphore_signal(barrier, 1, device_id=device, device_id_type=MESH)

    each(lambda d: signal(seq=partner(d)[1]))
    for k in range(1, parts):
        signal(tp=(part + k) % parts)
    has_next, has_last = group + 1 < groups, group > 0
    ends_group, opens_group = place == SUPER - 1, place == 0
    pl.when(has_next)(lambda: signal(seq=me + SUPER))
    pl.when(has_last)(lambda: signal(seq=me - SUPER))
    pl.when(has_next & ends_group)(lambda: signal(seq=me + 1))
    pl.when(has_last & opens_group)(lambda: signal(seq=me - 1))

    first = me * tokens
    starts, at = [], jnp.int32(0)
    for k in range(docs_ref.shape[0]):
        starts.append(at)
        at = at + docs_ref[k]

    def locate(position):
        found = jnp.zeros_like(position)
        for start in starts:
            found = jnp.maximum(found, jnp.where(position >= start, start, 0))
        return found

    position = first + lax.broadcasted_iota(jnp.int32, (tokens, 128), 0)
    doc = locate(position)
    doc_row = locate(first + lax.broadcasted_iota(jnp.int32, (8, tokens), 1))
    doc_last = doc_row[0:1, tokens - 1 : tokens]

    steps[...] = jnp.zeros_like(steps)
    steps[:, :heads] = jax.nn.softplus(step_ref[...] + bias_ref[...])
    rates = jnp.concatenate([rate_ref[...], jnp.zeros((1, 128 - heads), F32)], 1)
    log_decay = -steps[...] * rates
    order = lax.broadcasted_iota(jnp.int32, (tokens, tokens), 0)
    across = lax.broadcasted_iota(jnp.int32, (tokens, tokens), 1)
    lower = across <= order
    cumulated = jnp.dot(
        lower.astype(F32), log_decay, precision=EXACT, preferred_element_type=F32
    )
    grown = jnp.exp(cumulated)
    shrunk = jnp.exp(-cumulated) * steps[...]
    last = grown[tokens - 1 : tokens, :]
    rows_c[...] = shrunk.T
    weights = jnp.where(doc == doc_last, shrunk * last, 0.0)
    opened = jnp.where(doc < first, grown, 0.0)
    factor[...] = opened[tokens - 1 : tokens, :]

    count = (
        SUPER - 1 + parts - 1 + has_next.astype(jnp.int32) + has_last.astype(jnp.int32)
        + (has_next & ends_group).astype(jnp.int32) + (has_last & opens_group).astype(jnp.int32)
    )
    pl.semaphore_wait(barrier, count)

    def halo_copies():
        return [
            remote(
                ref.at[pl.ds(tokens - 16, 16), :], halo.at[k], h_send.at[k], h_recv.at[k],
                seq=me + 1,
            )
            for k, ref in enumerate((b_ref, c_ref))
        ]

    @pl.when(me + 1 < shards)
    def _():
        for copy in halo_copies():
            copy.start()

    def f_copy(d):
        return remote(factor, fr.at[place], f_send.at[d], f_recv.at[d], seq=partner(d)[1])

    def e_copy(d):
        to, there = partner(d)
        source = ends.at[
            pl.ds(pl.multiple_of((to % 16) * rows, 8), rows),
            pl.ds(pl.multiple_of((to // 16) * lanes, 128), lanes),
        ]
        return remote(source, er.at[place], e_send.at[d], e_recv.at[d], seq=there)

    def q_copy(d):
        to, there = partner(d)
        return remote(qs.at[to], qr.at[place], q_send.at[d], q_recv.at[d], seq=there)

    each(lambda d: f_copy(d).start())

    low = lax.broadcasted_iota(jnp.int32, (tokens, 128), 1) < width

    def spread(columns, pair):
        one = jnp.broadcast_to(columns[:, 2 * pair : 2 * pair + 1], (tokens, 128))
        two = jnp.broadcast_to(columns[:, 2 * pair + 1 : 2 * pair + 2], (tokens, 128))
        return jnp.where(low, one, two)

    x_in.wait()
    for pair in range(pairs):
        cut = slice(128 * pair, 128 * pair + 128)
        weighted[:, cut] = (x[:, cut].astype(F32) * spread(weights, pair)).astype(BF16)

    ext[8:, :state] = b_ref[...].astype(F32)
    ext[8:, state:] = c_ref[...].astype(F32)

    @pl.when(me > 0)
    def _():
        for copy in halo_copies():
            copy.wait_recv()

    @pl.when(me == 0)
    def _():
        halo[...] = jnp.zeros_like(halo)

    ext[:8, :state] = halo[0].astype(F32)[8:]
    ext[:8, state:] = halo[1].astype(F32)[8:]

    def convolve(half):
        cut = slice(half * state, half * state + state)
        total = jnp.broadcast_to(shift_ref[:, cut], (tokens, state))
        for k in range(4):
            back = 3 - k
            term = taps_ref[k : k + 1, cut] * ext[8 - back : 8 - back + tokens, cut]
            total = total + jnp.where(position - back >= doc, term, 0.0)
        return total * jax.nn.sigmoid(total)

    b_turned = convolve(0).T.astype(BF16)
    ends[...] = jnp.dot(b_turned, weighted[...], preferred_element_type=F32)
    each(lambda d: e_copy(d).start())
    fr[place] = factor[...]
    er[place] = ends[
        pl.ds(pl.multiple_of((place % 16) * rows, 8), rows),
        pl.ds(pl.multiple_of((place // 16) * lanes, 128), lanes),
    ]

    c_conv[...] = convolve(1).astype(BF16)
    products = jnp.dot(c_conv[...], b_turned, preferred_element_type=F32)
    doc_wide = jnp.concatenate([doc, doc], 1)
    products = jnp.where(lower & (doc_row[0:1, :] == doc_wide), products, 0.0)
    half = tokens // 2
    top, bottom = products[:half, :half], products[half:, :]
    gate_in.wait()
    for pair in range(pairs):
        cut = slice(128 * pair, 128 * pair + 128)
        found = []
        for h in (2 * pair, 2 * pair + 1):
            decay = jnp.broadcast_to(grown[:, h : h + 1], (tokens, 128))
            row = rows_c[h : h + 1, :]
            low_scores = top * row[:, :half] * decay[:half]
            high = jnp.concatenate([decay[half:], decay[half:]], 1)
            high_scores = bottom * row * high
            found.append(
                jnp.concatenate(
                    [
                        jnp.dot(
                            low_scores.astype(BF16), x[:half, cut], preferred_element_type=F32
                        ),
                        jnp.dot(
                            high_scores.astype(BF16), x[:, cut], preferred_element_type=F32
                        ),
                    ],
                    0,
                )
            )
        opening = gate[:, cut].astype(F32)
        opening = opening * jax.nn.sigmoid(opening)
        dg[:, cut] = jnp.where(low, found[0], found[1]) * opening
        rs[:, cut] = spread(opened, pair) * opening

    each(lambda d: f_copy(d).wait())
    column = lax.broadcasted_iota(jnp.int32, (128, lanes), 1) // width
    column = column + (place // 16) * (lanes // width)
    pick = (column == lax.broadcasted_iota(jnp.int32, (128, lanes), 0)).astype(F32)
    gathered = jnp.concatenate([fr[k] for k in range(SUPER)], 0)
    wide[...] = jnp.dot(gathered, pick, precision=EXACT, preferred_element_type=F32)
    each(lambda d: e_copy(d).wait())

    def factor_of(k):
        return jnp.broadcast_to(wide[k : k + 1, :], (rows, lanes))

    total, scale = er[0], factor_of(0)
    for k in range(1, SUPER):
        total = factor_of(k) * total + er[k]
        scale = factor_of(k) * scale

    def z_copy():
        return remote(carry_out, carry_in, z_send, z_recv, seq=me + SUPER)

    @pl.when(has_last)
    def _():
        z_copy().wait_recv()

    @pl.when(group == 0)
    def _():
        carry_in[...] = jnp.zeros_like(carry_in)

    current = carry_in[...]
    carry_out[...] = scale * current + total

    @pl.when(has_next)
    def _():
        z_copy().start()

    for k in range(SUPER):
        qs[k] = current.astype(BF16)
        if k + 1 < SUPER:
            current = factor_of(k) * current + er[k]
    each(lambda d: q_copy(d).start())
    qr[place] = qs[place]

    @pl.when(has_next)
    def _():
        z_copy().wait_send()

    @pl.when(me + 1 < shards)
    def _():
        for copy in halo_copies():
            copy.wait_send()

    each(lambda d: q_copy(d).wait())
    for side in range(2):
        for k in range(0, 16, 2):
            both = [qr[side * 16 + k + u].astype(F32) for u in range(2)]
            q[k * rows : (k + 2) * rows, side * lanes : (side + 1) * lanes] = jnp.concatenate(
                both, 0
            ).astype(BF16)

    squares = jnp.zeros((tokens, 128), F32)
    for pair in range(pairs):
        cut = slice(128 * pair, 128 * pair + 128)
        from_state = jnp.dot(c_conv[...], q[:, cut], preferred_element_type=F32)
        gated = dg[:, cut] + from_state * rs[:, cut]
        dg[:, cut] = gated
        squares = squares + gated * gated
    sums[...] = jnp.sum(squares.T, axis=0, keepdims=True)
    copies = [
        remote(sums, others.at[k - 1], s_send.at[k - 1], s_recv.at[k - 1], tp=(part + k) % parts)
        for k in range(1, parts)
    ]
    for copy in copies:
        copy.start()
    for copy in copies:
        copy.wait()
    mean_square = (sums[...] + others[0] + others[1] + others[2]) * (1.0 / (features * parts))
    inverse = lax.rsqrt(mean_square + EPS)
    inverse = jnp.broadcast_to(inverse, (128, tokens)).T
    for pair in range(pairs):
        cut = slice(128 * pair, 128 * pair + 128)
        out_ref[:, cut] = (dg[:, cut] * inverse * gain_ref[:, cut]).astype(BF16)


def body(
    inputs, gate_input, b_source, c_source, step_raw, step_bias, decay_rate,
    conv_weight, conv_bias, norm_gain, doc_lengths,
):
    groups, parts = lax.axis_size("seq") // SUPER, lax.axis_size("tp")
    tokens, features = inputs.shape
    heads, state = step_raw.shape[1], b_source.shape[1]
    rows, lanes = state // 16, features // 2
    dma = pltpu.SemaphoreType.DMA
    vmem = pltpu.VMEM
    whole = pl.BlockSpec(memory_space=pltpu.VMEM)
    far = pl.BlockSpec(memory_space=pl.ANY)
    return pl.pallas_call(
        functools.partial(layer_kernel, groups, parts, heads),
        out_shape=jax.ShapeDtypeStruct((tokens, features), BF16),
        in_specs=[far, far] + [whole] * 8 + [pl.BlockSpec(memory_space=pltpu.SMEM)],
        out_specs=whole,
        scratch_shapes=[
            vmem((tokens, features), BF16),
            vmem((tokens, features), BF16),
            vmem((tokens, 128), F32),
            vmem((8 + tokens, 2 * state), F32),
            vmem((2, 16, state), BF16),
            vmem((tokens, features), BF16),
            vmem((tokens, state), BF16),
            vmem((128, tokens), F32),
            vmem((1, 128), F32),
            vmem((state, features), F32),
            vmem((SUPER, rows, lanes), F32),
            vmem((SUPER, 1, 128), F32),
            vmem((SUPER, lanes), F32),
            vmem((rows, lanes), F32),
            vmem((rows, lanes), F32),
            vmem((SUPER, rows, lanes), BF16),
            vmem((SUPER, rows, lanes), BF16),
            vmem((state, features), BF16),
            vmem((tokens, features), F32),
            vmem((tokens, features), F32),
            vmem((1, tokens), F32),
            vmem((parts - 1, 1, tokens), F32),
            dma((2,)), dma((2,)), dma((2,)), dma((SUPER,)), dma((SUPER,)), dma((SUPER,)),
            dma((SUPER,)), dma, dma, dma((SUPER,)), dma((SUPER,)),
            dma((parts - 1,)), dma((parts - 1,)),
        ],
        compiler_params=pltpu.CompilerParams(
            collective_id=0, has_side_effects=True, vmem_limit_bytes=48 * 1024 * 1024
        ),
    )(
        inputs, gate_input, b_source, c_source, step_raw, step_bias[None, :],
        decay_rate[None, :], conv_weight, conv_bias[None, :], norm_gain[None, :], doc_lengths,
    )


def solution(mesh):
    both, seq = P("seq", "tp"), P("seq", None)
    return jax.shard_map(
        body, mesh=mesh,
        in_specs=(both, both, seq, seq, both, P("tp"), P("tp"), P(), P(), P("tp"), P()),
        out_specs=both, check_vma=False,
    )
```

```python
import functools

import jax
import jax.numpy as jnp
from jax import lax
from jax.experimental import pallas as pl
from jax.experimental.pallas import tpu as pltpu
from jax.sharding import PartitionSpec as P

MESH = pl.DeviceIdType.MESH
EPS = 1e-05
SUPER = 32
F32 = jnp.float32
BF16 = jnp.bfloat16
EXACT = lax.Precision.HIGHEST


def remote(source, target, send, recv, **device):
    return pltpu.make_async_remote_copy(
        source, target, send, recv, device_id=device, device_id_type=MESH
    )


def layer_kernel(
    groups, parts, heads,
    x_hbm, gate_hbm, b_hbm, c_hbm, step_hbm, bias_hbm, rate_hbm, taps_hbm, shift_hbm, gain_hbm,
    docs_hbm, out_ref,
    x, gate, b_ref, c_ref, step_ref, bias_ref, rate_ref, taps_ref, shift_ref, gain_ref, docs_ref,
    turned, ext, halo, weighted, c_conv, rows_c, factor, ends, er, fr, wide,
    z_factor, z_factors, z_total, z_totals, qs, qr, q, dg, rs, sums, others,
    in_sem, h_send, h_recv, f_send, f_recv, e_send, e_recv, z_send, z_recv, zf_send, zf_recv,
    q_send, q_recv, s_send, s_recv, ready,
):
    me, part = lax.axis_index("seq"), lax.axis_index("tp")
    shards = groups * SUPER
    group, place = me // SUPER, me % SUPER
    dz, dy, dx = place // 16, (place // 4) % 4, place % 4
    tokens, features = x.shape
    state = b_ref.shape[1]
    rows, lanes = er.shape[1], er.shape[2]
    width = features // heads
    pairs = features // 128

    def partner(d):
        to = ((dz + d // 16) % 2) * 16 + ((dy + (d // 4) % 4) % 4) * 4 + (dx + d % 4) % 4
        return to, group * SUPER + to

    def hops(d):
        along_y, along_x = (d // 4) % 4, d % 4
        return d // 16 + min(along_y, 4 - along_y) + min(along_x, 4 - along_x)

    farthest_first = sorted(range(1, SUPER), key=lambda d: (-hops(d), d % 4, d))

    def each(f):
        for d in farthest_first:
            f(d)

    barrier = pltpu.get_barrier_semaphore()

    def signal(**device):
        pl.semaphore_signal(barrier, 1, device_id=device, device_id_type=MESH)

    each(lambda d: signal(seq=partner(d)[1]))
    for k in range(1, parts):
        signal(tp=(part + k) % parts)
    has_next, has_last = group + 1 < groups, group > 0
    ends_group, opens_group = place == SUPER - 1, place == 0
    pl.when(has_next)(lambda: signal(seq=me + SUPER))
    pl.when(has_last)(lambda: signal(seq=me - SUPER))
    pl.when(has_next & ends_group)(lambda: signal(seq=me + 1))
    pl.when(has_last & opens_group)(lambda: signal(seq=me - 1))

    def fetch(k, source, target):
        copy = pltpu.make_async_copy(source, target, in_sem.at[k])
        copy.start()
        return copy

    step_in = fetch(0, step_hbm, step_ref)
    bias_in = fetch(1, bias_hbm, bias_ref)
    rate_in = fetch(2, rate_hbm, rate_ref)
    docs_in = fetch(3, docs_hbm, docs_ref)
    b_in = fetch(4, b_hbm, b_ref)
    c_in = fetch(5, c_hbm, c_ref)
    x_in = fetch(6, x_hbm, x)
    taps_in = fetch(7, taps_hbm, taps_ref)
    shift_in = fetch(8, shift_hbm, shift_ref)
    gate_in = fetch(9, gate_hbm, gate)
    gain_in = fetch(10, gain_hbm, gain_ref)

    docs_in.wait()
    first = me * tokens
    starts, at = [], jnp.int32(0)
    for k in range(docs_ref.shape[0]):
        starts.append(at)
        at = at + docs_ref[k]

    def locate(position):
        found = jnp.zeros_like(position)
        for start in starts:
            found = jnp.maximum(found, jnp.where(position >= start, start, 0))
        return found

    position = first + lax.broadcasted_iota(jnp.int32, (tokens, 128), 0)
    doc = locate(position)
    doc_row = locate(first + lax.broadcasted_iota(jnp.int32, (8, tokens), 1))
    doc_last = doc_row[0:1, tokens - 1 : tokens]

    step_in.wait()
    bias_in.wait()
    rate_in.wait()
    same = lax.broadcasted_iota(jnp.int32, (heads, heads), 0) == lax.broadcasted_iota(
        jnp.int32, (heads, heads), 1
    )

    def upright(row):
        return jnp.sum(jnp.where(same, jnp.broadcast_to(row, (heads, heads)), 0.0), 1, keepdims=True)

    step = jax.nn.softplus(step_ref[...] + upright(bias_ref[...]))
    log_decay = -step * upright(rate_ref[...])
    order = lax.broadcasted_iota(jnp.int32, (tokens, tokens), 0)
    across = lax.broadcasted_iota(jnp.int32, (tokens, tokens), 1)
    lower = across <= order
    cumulated = jnp.dot(
        log_decay, (order <= across).astype(F32), precision=EXACT, preferred_element_type=F32
    )
    grown = jnp.exp(cumulated)
    shrunk = jnp.exp(-cumulated) * step
    rows_c[...] = shrunk
    turned[...] = jnp.zeros_like(turned)
    turned[:heads, :] = grown
    grown_c = turned[...].T
    opened_c = jnp.where(doc < first, grown_c, 0.0)
    factor[...] = opened_c[tokens - 1 : tokens, :]
    turned[:heads, :] = jnp.where(
        doc_row[0:1, :] == doc_last, shrunk * grown[:, tokens - 1 : tokens], 0.0
    )
    weights_c = turned[...].T

    count = (
        SUPER - 1 + parts - 1 + has_next.astype(jnp.int32) + has_last.astype(jnp.int32)
        + (has_next & ends_group).astype(jnp.int32) + (has_last & opens_group).astype(jnp.int32)
    )
    pl.semaphore_wait(barrier, count)
    b_in.wait()
    c_in.wait()

    def halo_copies():
        return [
            remote(
                ref.at[pl.ds(tokens - 16, 16), :], halo.at[k], h_send.at[k], h_recv.at[k],
                seq=me + 1,
            )
            for k, ref in enumerate((b_ref, c_ref))
        ]

    @pl.when(me + 1 < shards)
    def _():
        for copy in halo_copies():
            copy.start()

    def f_copy(d):
        return remote(factor, fr.at[place], f_send.at[d], f_recv.at[d], seq=partner(d)[1])

    def e_copy(d):
        to, there = partner(d)
        source = ends.at[
            pl.ds(pl.multiple_of((to % 16) * rows, 8), rows),
            pl.ds(pl.multiple_of((to // 16) * lanes, 128), lanes),
        ]
        return remote(source, er.at[place], e_send.at[d], e_recv.at[d], seq=there)

    def q_copy(d):
        to, there = partner(d)
        return remote(qs.at[to], qr.at[place], q_send.at[d], q_recv.at[d], seq=there)

    each(lambda d: f_copy(d).start())

    low = lax.broadcasted_iota(jnp.int32, (tokens, 128), 1) < width

    def spread(columns, pair):
        one = jnp.broadcast_to(columns[:, 2 * pair : 2 * pair + 1], (tokens, 128))
        two = jnp.broadcast_to(columns[:, 2 * pair + 1 : 2 * pair + 2], (tokens, 128))
        return jnp.where(low, one, two)

    x_in.wait()
    for pair in range(pairs):
        cut = slice(128 * pair, 128 * pair + 128)
        weighted[:, cut] = (x[:, cut].astype(F32) * spread(weights_c, pair)).astype(BF16)

    taps_in.wait()
    shift_in.wait()
    ext[8:, :state] = b_ref[...].astype(F32)
    ext[8:, state:] = c_ref[...].astype(F32)

    @pl.when(me > 0)
    def _():
        for copy in halo_copies():
            copy.wait_recv()

    @pl.when(me == 0)
    def _():
        halo[...] = jnp.zeros_like(halo)

    ext[:8, :state] = halo[0].astype(F32)[8:]
    ext[:8, state:] = halo[1].astype(F32)[8:]

    def convolve(half):
        cut = slice(half * state, half * state + state)
        total = jnp.broadcast_to(shift_ref[:, cut], (tokens, state))
        for k in range(4):
            back = 3 - k
            term = taps_ref[k : k + 1, cut] * ext[8 - back : 8 - back + tokens, cut]
            total = total + jnp.where(position - back >= doc, term, 0.0)
        return total * jax.nn.sigmoid(total)

    b_turned = convolve(0).T.astype(BF16)
    ends[...] = jnp.dot(b_turned, weighted[...], preferred_element_type=F32)
    each(lambda d: e_copy(d).start())

    for k in range(2, groups):
        if k > 2:
            @pl.when(group + k - 1 < groups)
            def _():
                pl.semaphore_wait(ready.at[k - 1], 1)

        @pl.when(has_last & (group + k - 1 < groups))
        def _():
            pl.semaphore_signal(
                ready.at[k], 1, device_id={"seq": me - SUPER}, device_id_type=MESH
            )

    @pl.when(group + groups - 1 < groups)
    def _():
        pl.semaphore_wait(ready.at[groups - 1], 1)

    fr[place] = factor[...]
    er[place] = ends[
        pl.ds(pl.multiple_of((place % 16) * rows, 8), rows),
        pl.ds(pl.multiple_of((place // 16) * lanes, 128), lanes),
    ]

    c_conv[...] = convolve(1).astype(BF16)
    products = jnp.dot(c_conv[...], b_turned, preferred_element_type=F32)
    doc_wide = jnp.concatenate([doc, doc], 1)
    products = jnp.where(lower & (doc_row[0:1, :] == doc_wide), products, 0.0)
    half = tokens // 2
    top, bottom = products[:half, :half], products[half:, :]
    gate_in.wait()
    for pair in range(pairs):
        cut = slice(128 * pair, 128 * pair + 128)
        found = []
        for h in (2 * pair, 2 * pair + 1):
            decay = jnp.broadcast_to(grown_c[:, h : h + 1], (tokens, 128))
            row = rows_c[h : h + 1, :]
            low_scores = top * row[:, :half] * decay[:half]
            high = jnp.concatenate([decay[half:], decay[half:]], 1)
            high_scores = bottom * row * high
            found.append(
                jnp.concatenate(
                    [
                        jnp.dot(
                            low_scores.astype(BF16), x[:half, cut], preferred_element_type=F32
                        ),
                        jnp.dot(
                            high_scores.astype(BF16), x[:, cut], preferred_element_type=F32
                        ),
                    ],
                    0,
                )
            )
        opening = gate[:, cut].astype(F32)
        opening = opening * jax.nn.sigmoid(opening)
        dg[:, cut] = jnp.where(low, found[0], found[1]) * opening
        rs[:, cut] = spread(opened_c, pair) * opening

    each(lambda d: f_copy(d).wait())
    column = lax.broadcasted_iota(jnp.int32, (128, lanes), 1) // width
    column = column + (place // 16) * (lanes // width)
    pick = (column == lax.broadcasted_iota(jnp.int32, (128, lanes), 0)).astype(F32)
    gathered = jnp.concatenate([fr[k] for k in range(SUPER)], 0)
    wide[...] = jnp.dot(gathered, pick, precision=EXACT, preferred_element_type=F32)

    def zf_copy(k):
        there = me + k * SUPER
        return remote(z_factor, z_factors.at[group], zf_send.at[k], zf_recv.at[k], seq=there)

    def z_copy(k):
        there = me + k * SUPER
        return remote(z_total, z_totals.at[group], z_send.at[k], z_recv.at[k], seq=there)

    product = fr[0]
    for k in range(1, SUPER):
        product = product * fr[k]
    z_factor[...] = product
    for k in reversed(range(1, groups)):
        pl.when(group + k < groups)(lambda: zf_copy(k).start())
    each(lambda d: e_copy(d).wait())

    def factor_of(k):
        return jnp.broadcast_to(wide[k : k + 1, :], (rows, lanes))

    total = er[0]
    for k in range(1, SUPER):
        total = factor_of(k) * total + er[k]
    z_total[...] = total
    for k in reversed(range(1, groups)):
        pl.when(group + k < groups)(lambda: z_copy(k).start())
    for k in range(1, groups):
        @pl.when(group - k >= 0)
        def _():
            zf_copy(k).wait_recv()
            z_copy(k).wait_recv()

    passed = jnp.concatenate([z_factors[k] for k in range(groups)], 0)
    passed = jnp.concatenate([passed] * (8 // groups), 0)
    passed = jnp.dot(passed, pick, precision=EXACT, preferred_element_type=F32)
    current = jnp.zeros((rows, lanes), F32)
    for k in range(groups - 1):
        scale = jnp.broadcast_to(passed[k : k + 1, :], (rows, lanes))
        current = jnp.where(k < group, scale * current + z_totals[k], current)

    for k in range(SUPER):
        qs[k] = current.astype(BF16)
        if k + 1 < SUPER:
            current = factor_of(k) * current + er[k]
    each(lambda d: q_copy(d).start())
    qr[place] = qs[place]

    for k in range(1, groups):
        @pl.when(group + k < groups)
        def _():
            zf_copy(k).wait_send()
            z_copy(k).wait_send()

    @pl.when(me + 1 < shards)
    def _():
        for copy in halo_copies():
            copy.wait_send()

    each(lambda d: q_copy(d).wait())
    for side in range(2):
        for k in range(0, 16, 2):
            both = [qr[side * 16 + k + u].astype(F32) for u in range(2)]
            q[k * rows : (k + 2) * rows, side * lanes : (side + 1) * lanes] = jnp.concatenate(
                both, 0
            ).astype(BF16)

    squares = jnp.zeros((tokens, 128), F32)
    for pair in range(pairs):
        cut = slice(128 * pair, 128 * pair + 128)
        from_state = jnp.dot(c_conv[...], q[:, cut], preferred_element_type=F32)
        gated = dg[:, cut] + from_state * rs[:, cut]
        dg[:, cut] = gated
        squares = squares + gated * gated
    sums[...] = jnp.sum(squares.T, axis=0, keepdims=True)
    copies = [
        remote(sums, others.at[k - 1], s_send.at[k - 1], s_recv.at[k - 1], tp=(part + k) % parts)
        for k in range(1, parts)
    ]
    for copy in copies:
        copy.start()
    for copy in copies:
        copy.wait()
    mean_square = (sums[...] + others[0] + others[1] + others[2]) * (1.0 / (features * parts))
    inverse = lax.rsqrt(mean_square + EPS)
    inverse = jnp.broadcast_to(inverse, (128, tokens)).T
    gain_in.wait()
    for pair in range(pairs):
        cut = slice(128 * pair, 128 * pair + 128)
        out_ref[:, cut] = (dg[:, cut] * inverse * gain_ref[pair : pair + 1, :]).astype(BF16)


def body(
    inputs, gate_input, b_source, c_source, step_raw, step_bias, decay_rate,
    conv_weight, conv_bias, norm_gain, doc_lengths,
):
    groups, parts = lax.axis_size("seq") // SUPER, lax.axis_size("tp")
    tokens, features = inputs.shape
    heads, state = step_raw.shape[1], b_source.shape[1]
    rows, lanes = state // 16, features // 2
    dma = pltpu.SemaphoreType.DMA
    vmem = pltpu.VMEM
    far = pl.BlockSpec(memory_space=pltpu.HBM)
    return pl.pallas_call(
        functools.partial(layer_kernel, groups, parts, heads),
        out_shape=jax.ShapeDtypeStruct((tokens, features), BF16),
        in_specs=[far] * 11,
        out_specs=pl.BlockSpec(memory_space=pltpu.VMEM),
        scratch_shapes=[
            vmem((tokens, features), BF16),
            vmem((tokens, features), BF16),
            vmem((tokens, state), BF16),
            vmem((tokens, state), BF16),
            vmem((heads, tokens), F32),
            vmem((1, heads), F32),
            vmem((1, heads), F32),
            vmem(conv_weight.shape, F32),
            vmem((1, 2 * state), F32),
            vmem((features // 128, 128), F32),
            pltpu.SMEM(doc_lengths.shape, jnp.int32),
            vmem((128, tokens), F32),
            vmem((8 + tokens, 2 * state), F32),
            vmem((2, 16, state), BF16),
            vmem((tokens, features), BF16),
            vmem((tokens, state), BF16),
            vmem((heads, tokens), F32),
            vmem((1, 128), F32),
            vmem((state, features), F32),
            vmem((SUPER, rows, lanes), F32),
            vmem((SUPER, 1, 128), F32),
            vmem((SUPER, lanes), F32),
            vmem((1, 128), F32),
            vmem((groups, 1, 128), F32),
            vmem((rows, lanes), F32),
            vmem((groups, rows, lanes), F32),
            vmem((SUPER, rows, lanes), BF16),
            vmem((SUPER, rows, lanes), BF16),
            vmem((state, features), BF16),
            vmem((tokens, features), F32),
            vmem((tokens, features), F32),
            vmem((1, tokens), F32),
            vmem((parts - 1, 1, tokens), F32),
            dma((11,)), dma((2,)), dma((2,)), dma((SUPER,)), dma((SUPER,)), dma((SUPER,)),
            dma((SUPER,)), dma((groups,)), dma((groups,)), dma((groups,)), dma((groups,)),
            dma((SUPER,)), dma((SUPER,)), dma((parts - 1,)), dma((parts - 1,)),
            pltpu.SemaphoreType.REGULAR((groups,)),
        ],
        compiler_params=pltpu.CompilerParams(
            collective_id=0, has_side_effects=True, vmem_limit_bytes=67043328
        ),
    )(
        inputs, gate_input, b_source, c_source, step_raw.T, step_bias[None, :],
        decay_rate[None, :], conv_weight, conv_bias[None, :],
        norm_gain.reshape(features // 128, 128), doc_lengths,
    )


def solution(mesh):
    both, seq = P("seq", "tp"), P("seq", None)
    return jax.shard_map(
        body, mesh=mesh,
        in_specs=(both, both, seq, seq, both, P("tp"), P("tp"), P(), P(), P("tp"), P()),
        out_specs=both, check_vma=False,
    )
```

```python
import functools

import jax
import jax.numpy as jnp
from jax import lax
from jax.experimental import pallas as pl
from jax.experimental.pallas import tpu as pltpu
from jax.sharding import PartitionSpec as P

MESH = pl.DeviceIdType.MESH
EPS = 1e-05
SUPER = 32
F32 = jnp.float32
BF16 = jnp.bfloat16
EXACT = lax.Precision.HIGHEST


def remote(source, target, send, recv, **device):
    return pltpu.make_async_remote_copy(
        source, target, send, recv, device_id=device, device_id_type=MESH
    )


def layer_kernel(
    groups, parts, heads,
    x_hbm, gate_hbm, b_hbm, c_hbm, step_hbm, bias_hbm, rate_hbm, taps_hbm, shift_hbm, gain_hbm,
    docs_hbm, out_ref,
    x, gate, b_ref, c_ref, step_ref, bias_ref, rate_ref, taps_ref, shift_ref, gain_ref, docs_ref,
    turned, ext, halo, weighted, c_conv, rows_c, factor, ends, er, fr, wide,
    z_factor, z_factors, z_total, z_totals, qs, qr, q, dg, rs, sums, others,
    in_sem, h_send, h_recv, f_send, f_recv, e_send, e_recv, z_send, z_recv, zf_send, zf_recv,
    q_send, q_recv, s_send, s_recv, ready,
):
    me, part = lax.axis_index("seq"), lax.axis_index("tp")
    shards = groups * SUPER
    group, place = me // SUPER, me % SUPER
    dz, dy, dx = place // 16, (place // 4) % 4, place % 4
    tokens, features = x.shape
    state = b_ref.shape[1]
    rows, lanes = er.shape[1], er.shape[2]
    width = features // heads
    pairs = features // 128

    def partner(d):
        to = ((dz + d // 16) % 2) * 16 + ((dy + (d // 4) % 4) % 4) * 4 + (dx + d % 4) % 4
        return to, group * SUPER + to

    def hops(d):
        along_y, along_x = (d // 4) % 4, d % 4
        return d // 16 + min(along_y, 4 - along_y) + min(along_x, 4 - along_x)

    farthest_first = sorted(range(1, SUPER), key=lambda d: (-hops(d), d % 4, d))

    def each(f):
        for d in farthest_first:
            f(d)

    barrier = pltpu.get_barrier_semaphore()

    def signal(**device):
        pl.semaphore_signal(barrier, 1, device_id=device, device_id_type=MESH)

    each(lambda d: signal(seq=partner(d)[1]))
    for k in range(1, parts):
        signal(tp=(part + k) % parts)
    has_next, has_last = group + 1 < groups, group > 0
    ends_group, opens_group = place == SUPER - 1, place == 0
    pl.when(has_next)(lambda: signal(seq=me + SUPER))
    pl.when(has_last)(lambda: signal(seq=me - SUPER))
    pl.when(has_next & ends_group)(lambda: signal(seq=me + 1))
    pl.when(has_last & opens_group)(lambda: signal(seq=me - 1))

    def fetch(k, source, target):
        copy = pltpu.make_async_copy(source, target, in_sem.at[k])
        copy.start()
        return copy

    b_in = fetch(4, b_hbm, b_ref)
    c_in = fetch(5, c_hbm, c_ref)
    step_in = fetch(0, step_hbm, step_ref)
    bias_in = fetch(1, bias_hbm, bias_ref)
    rate_in = fetch(2, rate_hbm, rate_ref)
    docs_in = fetch(3, docs_hbm, docs_ref)
    x_in = fetch(6, x_hbm, x)
    taps_in = fetch(7, taps_hbm, taps_ref)
    shift_in = fetch(8, shift_hbm, shift_ref)
    gate_in = fetch(9, gate_hbm, gate)
    gain_in = fetch(10, gain_hbm, gain_ref)

    count = (
        SUPER - 1 + parts - 1 + has_next.astype(jnp.int32) + has_last.astype(jnp.int32)
        + (has_next & ends_group).astype(jnp.int32) + (has_last & opens_group).astype(jnp.int32)
    )
    pl.semaphore_wait(barrier, count)
    b_in.wait()
    c_in.wait()

    def halo_copies():
        return [
            remote(
                ref.at[pl.ds(tokens - 16, 16), :], halo.at[k], h_send.at[k], h_recv.at[k],
                seq=me + 1,
            )
            for k, ref in enumerate((b_ref, c_ref))
        ]

    @pl.when(me + 1 < shards)
    def _():
        for copy in halo_copies():
            copy.start()

    docs_in.wait()
    first = me * tokens
    starts, at = [], jnp.int32(0)
    for k in range(docs_ref.shape[0]):
        starts.append(at)
        at = at + docs_ref[k]

    def locate(position):
        found = jnp.zeros_like(position)
        for start in starts:
            found = jnp.maximum(found, jnp.where(position >= start, start, 0))
        return found

    position = first + lax.broadcasted_iota(jnp.int32, (tokens, 128), 0)
    doc = locate(position)
    doc_row = locate(first + lax.broadcasted_iota(jnp.int32, (8, tokens), 1))
    doc_last = doc_row[0:1, tokens - 1 : tokens]

    step_in.wait()
    bias_in.wait()
    rate_in.wait()
    same = lax.broadcasted_iota(jnp.int32, (heads, heads), 0) == lax.broadcasted_iota(
        jnp.int32, (heads, heads), 1
    )

    def upright(row):
        return jnp.sum(jnp.where(same, jnp.broadcast_to(row, (heads, heads)), 0.0), 1, keepdims=True)

    step = jax.nn.softplus(step_ref[...] + upright(bias_ref[...]))
    log_decay = -step * upright(rate_ref[...])
    order = lax.broadcasted_iota(jnp.int32, (tokens, tokens), 0)
    across = lax.broadcasted_iota(jnp.int32, (tokens, tokens), 1)
    lower = across <= order
    cumulated = jnp.dot(
        log_decay, (order <= across).astype(F32), precision=EXACT, preferred_element_type=F32
    )
    grown = jnp.exp(cumulated)
    shrunk = jnp.exp(-cumulated) * step
    rows_c[...] = shrunk
    turned[...] = jnp.zeros_like(turned)
    turned[:heads, :] = grown
    grown_c = turned[...].T
    opened_c = jnp.where(doc < first, grown_c, 0.0)
    factor[...] = opened_c[tokens - 1 : tokens, :]
    turned[:heads, :] = jnp.where(
        doc_row[0:1, :] == doc_last, shrunk * grown[:, tokens - 1 : tokens], 0.0
    )
    weights_c = turned[...].T

    def f_copy(d):
        return remote(factor, fr.at[place], f_send, f_recv, seq=partner(d)[1])

    def e_copy(d):
        to, there = partner(d)
        source = ends.at[
            pl.ds(pl.multiple_of((to % 16) * rows, 8), rows),
            pl.ds(pl.multiple_of((to // 16) * lanes, 128), lanes),
        ]
        return remote(source, er.at[place], e_send, e_recv, seq=there)

    def q_copy(d):
        to, there = partner(d)
        return remote(qs.at[to], qr.at[place], q_send, q_recv, seq=there)

    def wait_all(buffer, *sems):
        part_of = buffer.at[pl.ds(0, SUPER - 1)]
        for sem in sems:
            pltpu.make_async_copy(part_of, part_of, sem).wait()

    each(lambda d: f_copy(d).start())

    low = lax.broadcasted_iota(jnp.int32, (tokens, 128), 1) < width

    def spread(columns, pair):
        one = jnp.broadcast_to(columns[:, 2 * pair : 2 * pair + 1], (tokens, 128))
        two = jnp.broadcast_to(columns[:, 2 * pair + 1 : 2 * pair + 2], (tokens, 128))
        return jnp.where(low, one, two)

    x_in.wait()
    for pair in range(pairs):
        cut = slice(128 * pair, 128 * pair + 128)
        weighted[:, cut] = (x[:, cut].astype(F32) * spread(weights_c, pair)).astype(BF16)

    taps_in.wait()
    shift_in.wait()
    ext[8:, :state] = b_ref[...].astype(F32)
    ext[8:, state:] = c_ref[...].astype(F32)

    @pl.when(me > 0)
    def _():
        for copy in halo_copies():
            copy.wait_recv()

    @pl.when(me == 0)
    def _():
        halo[...] = jnp.zeros_like(halo)

    ext[:8, :state] = halo[0].astype(F32)[8:]
    ext[:8, state:] = halo[1].astype(F32)[8:]

    def convolve(half):
        cut = slice(half * state, half * state + state)
        total = jnp.broadcast_to(shift_ref[:, cut], (tokens, state))
        for k in range(4):
            back = 3 - k
            term = taps_ref[k : k + 1, cut] * ext[8 - back : 8 - back + tokens, cut]
            total = total + jnp.where(position - back >= doc, term, 0.0)
        return total * jax.nn.sigmoid(total)

    b_turned = convolve(0).T.astype(BF16)
    ends[...] = jnp.dot(b_turned, weighted[...], preferred_element_type=F32)
    each(lambda d: e_copy(d).start())

    for k in range(2, groups):
        if k > 2:
            @pl.when(group + k - 1 < groups)
            def _():
                pl.semaphore_wait(ready.at[k - 1], 1)

        @pl.when(has_last & (group + k - 1 < groups))
        def _():
            pl.semaphore_signal(
                ready.at[k], 1, device_id={"seq": me - SUPER}, device_id_type=MESH
            )

    @pl.when(group + groups - 1 < groups)
    def _():
        pl.semaphore_wait(ready.at[groups - 1], 1)

    fr[place] = factor[...]
    er[place] = ends[
        pl.ds(pl.multiple_of((place % 16) * rows, 8), rows),
        pl.ds(pl.multiple_of((place // 16) * lanes, 128), lanes),
    ]

    c_conv[...] = convolve(1).astype(BF16)
    products = jnp.dot(c_conv[...], b_turned, preferred_element_type=F32)
    doc_wide = jnp.concatenate([doc, doc], 1)
    products = jnp.where(lower & (doc_row[0:1, :] == doc_wide), products, 0.0)
    half = tokens // 2
    top, bottom = products[:half, :half], products[half:, :]
    gate_in.wait()
    for pair in range(pairs):
        cut = slice(128 * pair, 128 * pair + 128)
        found = []
        for h in (2 * pair, 2 * pair + 1):
            decay = jnp.broadcast_to(grown_c[:, h : h + 1], (tokens, 128))
            row = rows_c[h : h + 1, :]
            low_scores = top * row[:, :half] * decay[:half]
            high = jnp.concatenate([decay[half:], decay[half:]], 1)
            high_scores = bottom * row * high
            found.append(
                jnp.concatenate(
                    [
                        jnp.dot(
                            low_scores.astype(BF16), x[:half, cut], preferred_element_type=F32
                        ),
                        jnp.dot(
                            high_scores.astype(BF16), x[:, cut], preferred_element_type=F32
                        ),
                    ],
                    0,
                )
            )
        opening = gate[:, cut].astype(F32)
        opening = opening * jax.nn.sigmoid(opening)
        dg[:, cut] = jnp.where(low, found[0], found[1]) * opening
        rs[:, cut] = spread(opened_c, pair) * opening

    wait_all(fr, f_send, f_recv)
    column = lax.broadcasted_iota(jnp.int32, (128, lanes), 1) // width
    column = column + (place // 16) * (lanes // width)
    pick = (column == lax.broadcasted_iota(jnp.int32, (128, lanes), 0)).astype(F32)
    gathered = jnp.concatenate([fr[k] for k in range(SUPER)], 0)
    wide[...] = jnp.dot(gathered, pick, precision=EXACT, preferred_element_type=F32)

    def zf_copy(k):
        there = me + k * SUPER
        return remote(z_factor, z_factors.at[group], zf_send.at[k], zf_recv.at[k], seq=there)

    def z_copy(k):
        there = me + k * SUPER
        return remote(z_total, z_totals.at[group], z_send.at[k], z_recv.at[k], seq=there)

    product = fr[0]
    for k in range(1, SUPER):
        product = product * fr[k]
    z_factor[...] = product
    for k in reversed(range(1, groups)):
        pl.when(group + k < groups)(lambda: zf_copy(k).start())
    wait_all(er, e_send, e_recv)

    def factor_of(k):
        return jnp.broadcast_to(wide[k : k + 1, :], (rows, lanes))

    total = er[0]
    for k in range(1, SUPER):
        total = factor_of(k) * total + er[k]
    z_total[...] = total
    for k in reversed(range(1, groups)):
        pl.when(group + k < groups)(lambda: z_copy(k).start())
    for k in range(1, groups):
        @pl.when(group - k >= 0)
        def _():
            zf_copy(k).wait_recv()
            z_copy(k).wait_recv()

    passed = jnp.concatenate([z_factors[k] for k in range(groups)], 0)
    passed = jnp.concatenate([passed] * (8 // groups), 0)
    passed = jnp.dot(passed, pick, precision=EXACT, preferred_element_type=F32)
    current = jnp.zeros((rows, lanes), F32)
    for k in range(groups - 1):
        scale = jnp.broadcast_to(passed[k : k + 1, :], (rows, lanes))
        current = jnp.where(k < group, scale * current + z_totals[k], current)

    for k in range(SUPER):
        qs[k] = current.astype(BF16)
        if k + 1 < SUPER:
            current = factor_of(k) * current + er[k]
    each(lambda d: q_copy(d).start())
    qr[place] = qs[place]

    for k in range(1, groups):
        @pl.when(group + k < groups)
        def _():
            zf_copy(k).wait_send()
            z_copy(k).wait_send()

    @pl.when(me + 1 < shards)
    def _():
        for copy in halo_copies():
            copy.wait_send()

    wait_all(qr, q_send, q_recv)
    for side in range(2):
        for k in range(0, 16, 2):
            both = [qr[side * 16 + k + u].astype(F32) for u in range(2)]
            q[k * rows : (k + 2) * rows, side * lanes : (side + 1) * lanes] = jnp.concatenate(
                both, 0
            ).astype(BF16)

    squares = jnp.zeros((tokens, 128), F32)
    for pair in range(pairs):
        cut = slice(128 * pair, 128 * pair + 128)
        from_state = jnp.dot(c_conv[...], q[:, cut], preferred_element_type=F32)
        gated = dg[:, cut] + from_state * rs[:, cut]
        dg[:, cut] = gated
        squares = squares + gated * gated
    sums[...] = jnp.sum(squares.T, axis=0, keepdims=True)
    copies = [
        remote(sums, others.at[k - 1], s_send.at[k - 1], s_recv.at[k - 1], tp=(part + k) % parts)
        for k in range(1, parts)
    ]
    for copy in copies:
        copy.start()
    for copy in copies:
        copy.wait()
    mean_square = (sums[...] + others[0] + others[1] + others[2]) * (1.0 / (features * parts))
    inverse = lax.rsqrt(mean_square + EPS)
    inverse = jnp.broadcast_to(inverse, (128, tokens)).T
    gain_in.wait()
    for pair in range(pairs):
        cut = slice(128 * pair, 128 * pair + 128)
        out_ref[:, cut] = (dg[:, cut] * inverse * gain_ref[pair : pair + 1, :]).astype(BF16)


def body(
    inputs, gate_input, b_source, c_source, step_raw, step_bias, decay_rate,
    conv_weight, conv_bias, norm_gain, doc_lengths,
):
    groups, parts = lax.axis_size("seq") // SUPER, lax.axis_size("tp")
    tokens, features = inputs.shape
    heads, state = step_raw.shape[1], b_source.shape[1]
    rows, lanes = state // 16, features // 2
    dma = pltpu.SemaphoreType.DMA
    vmem = pltpu.VMEM
    far = pl.BlockSpec(memory_space=pltpu.HBM)
    pinned = [
        pltpu.with_memory_space_constraint(a, pltpu.HBM)
        for a in (
            inputs, gate_input, b_source, c_source, step_raw.T, step_bias[None, :],
            decay_rate[None, :], conv_weight, conv_bias[None, :],
            norm_gain.reshape(features // 128, 128), doc_lengths,
        )
    ]
    return pl.pallas_call(
        functools.partial(layer_kernel, groups, parts, heads),
        out_shape=jax.ShapeDtypeStruct((tokens, features), BF16),
        in_specs=[far] * 11,
        out_specs=pl.BlockSpec(memory_space=pltpu.VMEM),
        scratch_shapes=[
            vmem((tokens, features), BF16),
            vmem((tokens, features), BF16),
            vmem((tokens, state), BF16),
            vmem((tokens, state), BF16),
            vmem((heads, tokens), F32),
            vmem((1, heads), F32),
            vmem((1, heads), F32),
            vmem(conv_weight.shape, F32),
            vmem((1, 2 * state), F32),
            vmem((features // 128, 128), F32),
            pltpu.SMEM(doc_lengths.shape, jnp.int32),
            vmem((128, tokens), F32),
            vmem((8 + tokens, 2 * state), F32),
            vmem((2, 16, state), BF16),
            vmem((tokens, features), BF16),
            vmem((tokens, state), BF16),
            vmem((heads, tokens), F32),
            vmem((1, 128), F32),
            vmem((state, features), F32),
            vmem((SUPER, rows, lanes), F32),
            vmem((SUPER, 1, 128), F32),
            vmem((SUPER, lanes), F32),
            vmem((1, 128), F32),
            vmem((groups, 1, 128), F32),
            vmem((rows, lanes), F32),
            vmem((groups, rows, lanes), F32),
            vmem((SUPER, rows, lanes), BF16),
            vmem((SUPER, rows, lanes), BF16),
            vmem((state, features), BF16),
            vmem((tokens, features), F32),
            vmem((tokens, features), F32),
            vmem((1, tokens), F32),
            vmem((parts - 1, 1, tokens), F32),
            dma((11,)), dma((2,)), dma((2,)), dma, dma, dma, dma,
            dma((groups,)), dma((groups,)), dma((groups,)), dma((groups,)),
            dma, dma, dma((parts - 1,)), dma((parts - 1,)),
            pltpu.SemaphoreType.REGULAR((groups,)),
        ],
        compiler_params=pltpu.CompilerParams(
            collective_id=0, has_side_effects=True, vmem_limit_bytes=48 * 1024 * 1024
        ),
    )(*pinned)


def solution(mesh):
    both, seq = P("seq", "tp"), P("seq", None)
    return jax.shard_map(
        body, mesh=mesh,
        in_specs=(both, both, seq, seq, both, P("tp"), P("tp"), P(), P(), P("tp"), P()),
        out_specs=both, check_vma=False,
    )
```

```python
import functools

import jax
import jax.numpy as jnp
from jax import lax
from jax.experimental import pallas as pl
from jax.experimental.pallas import tpu as pltpu
from jax.sharding import PartitionSpec as P

MESH = pl.DeviceIdType.MESH
EPS = 1e-05
SUPER = 32
F32 = jnp.float32
BF16 = jnp.bfloat16
EXACT = lax.Precision.HIGHEST


def remote(source, target, send, recv, **device):
    return pltpu.make_async_remote_copy(
        source, target, send, recv, device_id=device, device_id_type=MESH
    )


def layer_kernel(
    groups, parts, heads,
    x_hbm, gate_hbm, b_hbm, c_hbm, step_hbm, bias_hbm, rate_hbm, taps_hbm, shift_hbm, gain_hbm,
    docs_hbm, out_ref,
    x, gate, b_ref, c_ref, step_ref, bias_ref, rate_ref, taps_ref, shift_ref, gain_ref, docs_ref,
    turned, ext, halo, weighted, c_conv, rows_c, factor, ends, er, fr, wide,
    z_factor, z_factor_in, z_total, z_total_in, z_state, z_state_in, qs, qr, q, dg, rs, sums, others,
    in_sem, h_send, h_recv, f_send, f_recv, e_send, e_recv, z_send, z_recv,
    q_send, q_recv, s_send, s_recv, ready,
):
    me, part = lax.axis_index("seq"), lax.axis_index("tp")
    shards = groups * SUPER
    group, place = me // SUPER, me % SUPER
    dz, dy, dx = place // 16, (place // 4) % 4, place % 4
    tokens, features = x.shape
    state = b_ref.shape[1]
    rows, lanes = er.shape[1], er.shape[2]
    width = features // heads
    pairs = features // 128

    def partner(d):
        to = ((dz + d // 16) % 2) * 16 + ((dy + (d // 4) % 4) % 4) * 4 + (dx + d % 4) % 4
        return to, group * SUPER + to

    def hops(d):
        along_y, along_x = (d // 4) % 4, d % 4
        return d // 16 + min(along_y, 4 - along_y) + min(along_x, 4 - along_x)

    farthest_first = sorted(range(1, SUPER), key=lambda d: (-hops(d), d % 4, d))

    def each(f):
        for d in farthest_first:
            f(d)

    barrier = pltpu.get_barrier_semaphore()

    def signal(**device):
        pl.semaphore_signal(barrier, 1, device_id=device, device_id_type=MESH)

    has_next, has_last = group + 1 < groups, group > 0
    has_second = group + 2 < groups
    ends_group, opens_group = place == SUPER - 1, place == 0
    pl.when(has_last)(lambda: signal(seq=me - SUPER))
    pl.when(has_last & opens_group)(lambda: signal(seq=me - 1))
    each(lambda d: signal(seq=partner(d)[1]))
    pl.when(has_next)(lambda: signal(seq=me + SUPER))
    pl.when(has_next & ends_group)(lambda: signal(seq=me + 1))
    chip_mate = part // 2 * 2 + 1 - part % 2
    signal(tp=chip_mate)
    upper = part // 2

    def fetch(k, source, target):
        copy = pltpu.make_async_copy(source, target, in_sem.at[k])
        copy.start()
        return copy

    b_in = fetch(4, b_hbm, b_ref)
    c_in = fetch(5, c_hbm, c_ref)
    step_in = fetch(0, step_hbm, step_ref)
    bias_in = fetch(1, bias_hbm, bias_ref)
    rate_in = fetch(2, rate_hbm, rate_ref)
    docs_in = fetch(3, docs_hbm, docs_ref)
    x_in = fetch(6, x_hbm, x)
    taps_in = fetch(7, taps_hbm, taps_ref)
    shift_in = fetch(8, shift_hbm, shift_ref)
    gate_in = fetch(9, gate_hbm, gate)
    gain_in = fetch(10, gain_hbm, gain_ref)

    count = (
        SUPER - 1 + 1 + 2 * upper + has_next.astype(jnp.int32) + has_last.astype(jnp.int32)
        + (has_next & ends_group).astype(jnp.int32) + (has_last & opens_group).astype(jnp.int32)
    )
    pl.semaphore_wait(barrier, count)
    for core in range(2):
        signal(tp=(1 - upper) * 2 + core)
    @pl.when(has_last & has_next)
    def _():
        pl.semaphore_signal(ready, 1, device_id={"seq": me - SUPER}, device_id_type=MESH)

    b_in.wait()
    c_in.wait()

    def halo_copies():
        return [
            remote(
                ref.at[pl.ds(tokens - 16, 16), :], halo.at[k], h_send.at[k], h_recv.at[k],
                seq=me + 1,
            )
            for k, ref in enumerate((b_ref, c_ref))
        ]

    @pl.when(me + 1 < shards)
    def _():
        for copy in halo_copies():
            copy.start()

    docs_in.wait()
    first = me * tokens
    starts, at = [], jnp.int32(0)
    for k in range(docs_ref.shape[0]):
        starts.append(at)
        at = at + docs_ref[k]

    def locate(position):
        found = jnp.zeros_like(position)
        for start in starts:
            found = jnp.maximum(found, jnp.where(position >= start, start, 0))
        return found

    position = first + lax.broadcasted_iota(jnp.int32, (tokens, 128), 0)
    doc = locate(position)
    doc_row = locate(first + lax.broadcasted_iota(jnp.int32, (8, tokens), 1))
    doc_last = doc_row[0:1, tokens - 1 : tokens]

    step_in.wait()
    bias_in.wait()
    rate_in.wait()
    same = lax.broadcasted_iota(jnp.int32, (heads, heads), 0) == lax.broadcasted_iota(
        jnp.int32, (heads, heads), 1
    )

    def upright(row):
        return jnp.sum(jnp.where(same, jnp.broadcast_to(row, (heads, heads)), 0.0), 1, keepdims=True)

    step = jax.nn.softplus(step_ref[...] + upright(bias_ref[...]))
    log_decay = -step * upright(rate_ref[...])
    order = lax.broadcasted_iota(jnp.int32, (tokens, tokens), 0)
    across = lax.broadcasted_iota(jnp.int32, (tokens, tokens), 1)
    lower = across <= order
    cumulated = jnp.dot(
        log_decay, (order <= across).astype(F32), precision=EXACT, preferred_element_type=F32
    )
    grown = jnp.exp(cumulated)
    shrunk = jnp.exp(-cumulated) * step
    rows_c[...] = shrunk
    turned[...] = jnp.zeros_like(turned)
    turned[:heads, :] = grown
    grown_c = turned[...].T
    opened_c = jnp.where(doc < first, grown_c, 0.0)
    factor[...] = opened_c[tokens - 1 : tokens, :]
    turned[:heads, :] = jnp.where(
        doc_row[0:1, :] == doc_last, shrunk * grown[:, tokens - 1 : tokens], 0.0
    )
    weights_c = turned[...].T

    def f_copy(d):
        return remote(factor, fr.at[place], f_send, f_recv, seq=partner(d)[1])

    def e_copy(d):
        to, there = partner(d)
        source = ends.at[
            pl.ds(pl.multiple_of((to % 16) * rows, 8), rows),
            pl.ds(pl.multiple_of((to // 16) * lanes, 128), lanes),
        ]
        return remote(source, er.at[place], e_send, e_recv, seq=there)

    def q_copy(d):
        to, there = partner(d)
        return remote(qs.at[to], qr.at[place], q_send, q_recv, seq=there)

    def wait_all(buffer, *sems):
        part_of = buffer.at[pl.ds(0, SUPER - 1)]
        for sem in sems:
            pltpu.make_async_copy(part_of, part_of, sem).wait()

    each(lambda d: f_copy(d).start())

    low = lax.broadcasted_iota(jnp.int32, (tokens, 128), 1) < width

    def spread(columns, pair):
        one = jnp.broadcast_to(columns[:, 2 * pair : 2 * pair + 1], (tokens, 128))
        two = jnp.broadcast_to(columns[:, 2 * pair + 1 : 2 * pair + 2], (tokens, 128))
        return jnp.where(low, one, two)

    x_in.wait()
    for pair in range(pairs):
        cut = slice(128 * pair, 128 * pair + 128)
        weighted[:, cut] = (x[:, cut].astype(F32) * spread(weights_c, pair)).astype(BF16)

    taps_in.wait()
    shift_in.wait()
    ext[8:, :state] = b_ref[...].astype(F32)
    ext[8:, state:] = c_ref[...].astype(F32)

    @pl.when(me > 0)
    def _():
        for copy in halo_copies():
            copy.wait_recv()

    @pl.when(me == 0)
    def _():
        halo[...] = jnp.zeros_like(halo)

    ext[:8, :state] = halo[0].astype(F32)[8:]
    ext[:8, state:] = halo[1].astype(F32)[8:]

    def convolve(half):
        cut = slice(half * state, half * state + state)
        total = jnp.broadcast_to(shift_ref[:, cut], (tokens, state))
        for k in range(4):
            back = 3 - k
            term = taps_ref[k : k + 1, cut] * ext[8 - back : 8 - back + tokens, cut]
            total = total + jnp.where(position - back >= doc, term, 0.0)
        return total * jax.nn.sigmoid(total)

    b_turned = convolve(0).T.astype(BF16)
    ends[...] = jnp.dot(b_turned, weighted[...], preferred_element_type=F32)
    each(lambda d: e_copy(d).start())

    fr[place] = factor[...]
    er[place] = ends[
        pl.ds(pl.multiple_of((place % 16) * rows, 8), rows),
        pl.ds(pl.multiple_of((place // 16) * lanes, 128), lanes),
    ]

    c_conv[...] = convolve(1).astype(BF16)
    products = jnp.dot(c_conv[...], b_turned, preferred_element_type=F32)
    doc_wide = jnp.concatenate([doc, doc], 1)
    products = jnp.where(lower & (doc_row[0:1, :] == doc_wide), products, 0.0)
    half = tokens // 2
    top, bottom = products[:half, :half], products[half:, :]
    gate_in.wait()
    for pair in range(pairs):
        cut = slice(128 * pair, 128 * pair + 128)
        found = []
        for h in (2 * pair, 2 * pair + 1):
            decay = jnp.broadcast_to(grown_c[:, h : h + 1], (tokens, 128))
            row = rows_c[h : h + 1, :]
            low_scores = top * row[:, :half] * decay[:half]
            high = jnp.concatenate([decay[half:], decay[half:]], 1)
            high_scores = bottom * row * high
            found.append(
                jnp.concatenate(
                    [
                        jnp.dot(
                            low_scores.astype(BF16), x[:half, cut], preferred_element_type=F32
                        ),
                        jnp.dot(
                            high_scores.astype(BF16), x[:, cut], preferred_element_type=F32
                        ),
                    ],
                    0,
                )
            )
        opening = gate[:, cut].astype(F32)
        opening = opening * jax.nn.sigmoid(opening)
        dg[:, cut] = jnp.where(low, found[0], found[1]) * opening
        rs[:, cut] = spread(opened_c, pair) * opening

    wait_all(fr, f_send, f_recv)
    column = lax.broadcasted_iota(jnp.int32, (128, lanes), 1) // width
    column = column + (place // 16) * (lanes // width)
    pick = (column == lax.broadcasted_iota(jnp.int32, (128, lanes), 0)).astype(F32)
    gathered = jnp.concatenate([fr[k] for k in range(SUPER)], 0)
    wide[...] = jnp.dot(gathered, pick, precision=EXACT, preferred_element_type=F32)

    product = fr[0]
    for k in range(1, SUPER):
        product = product * fr[k]
    z_factor[...] = product

    def factor_copy():
        return remote(z_factor, z_factor_in, z_send.at[0], z_recv.at[0], seq=me + SUPER)

    def total_copy():
        return remote(z_total, z_total_in, z_send.at[1], z_recv.at[1], seq=me + SUPER)

    def state_copy():
        return remote(z_state, z_state_in, z_send.at[2], z_recv.at[2], seq=me + 2 * SUPER)

    pl.when(has_next)(lambda: factor_copy().start())

    def expand(row):
        return jnp.dot(
            jnp.broadcast_to(row, (rows, 128)), pick, precision=EXACT, preferred_element_type=F32
        )

    scale = expand(product)
    wait_all(er, e_send, e_recv)

    def factor_of(k):
        return jnp.broadcast_to(wide[k : k + 1, :], (rows, lanes))

    total = er[0]
    for k in range(1, SUPER):
        total = factor_of(k) * total + er[k]
    z_total[...] = total
    pl.when(has_next)(lambda: total_copy().start())

    @pl.when(group < 2)
    def _():
        z_state_in[...] = jnp.zeros_like(z_state_in)

    @pl.when(group == 0)
    def _():
        z_factor_in[...] = jnp.zeros_like(z_factor_in)
        z_total_in[...] = jnp.zeros_like(z_total_in)

    @pl.when(has_last)
    def _():
        factor_copy().wait_recv()
        total_copy().wait_recv()

    scale_in = expand(z_factor_in[...])

    @pl.when(group > 1)
    def _():
        state_copy().wait_recv()

    current = scale_in * z_state_in[...] + z_total_in[...]
    z_state[...] = scale * current + total

    @pl.when(has_second)
    def _():
        pl.semaphore_wait(ready, 1)
        state_copy().start()

    for k in range(SUPER):
        qs[k] = current.astype(BF16)
        if k + 1 < SUPER:
            current = factor_of(k) * current + er[k]
    each(lambda d: q_copy(d).start())
    qr[place] = qs[place]

    wait_all(qr, q_send, q_recv)
    for side in range(2):
        for k in range(0, 16, 2):
            both = [qr[side * 16 + k + u].astype(F32) for u in range(2)]
            q[k * rows : (k + 2) * rows, side * lanes : (side + 1) * lanes] = jnp.concatenate(
                both, 0
            ).astype(BF16)

    squares = jnp.zeros((tokens, 128), F32)
    for pair in range(pairs):
        cut = slice(128 * pair, 128 * pair + 128)
        from_state = jnp.dot(c_conv[...], q[:, cut], preferred_element_type=F32)
        gated = dg[:, cut] + from_state * rs[:, cut]
        dg[:, cut] = gated
        squares = squares + gated * gated
    sums[...] = jnp.sum(squares.T, axis=0, keepdims=True)
    copies = [
        remote(sums, others.at[k - 1], s_send.at[k - 1], s_recv.at[k - 1], tp=(part + k) % parts)
        for k in range(1, parts)
    ]
    @pl.when(upper == 0)
    def _():
        pl.semaphore_wait(barrier, 2)

    for copy in copies:
        copy.start()

    @pl.when(me + 1 < shards)
    def _():
        for copy in halo_copies():
            copy.wait_send()

    @pl.when(has_next)
    def _():
        factor_copy().wait_send()
        total_copy().wait_send()

    pl.when(has_second)(lambda: state_copy().wait_send())
    for copy in copies:
        copy.wait()
    mean_square = (sums[...] + others[0] + others[1] + others[2]) * (1.0 / (features * parts))
    inverse = lax.rsqrt(mean_square + EPS)
    inverse = jnp.broadcast_to(inverse, (128, tokens)).T
    gain_in.wait()
    for pair in range(pairs):
        cut = slice(128 * pair, 128 * pair + 128)
        out_ref[:, cut] = (dg[:, cut] * inverse * gain_ref[pair : pair + 1, :]).astype(BF16)


def body(
    inputs, gate_input, b_source, c_source, step_raw, step_bias, decay_rate,
    conv_weight, conv_bias, norm_gain, doc_lengths,
):
    groups, parts = lax.axis_size("seq") // SUPER, lax.axis_size("tp")
    tokens, features = inputs.shape
    heads, state = step_raw.shape[1], b_source.shape[1]
    rows, lanes = state // 16, features // 2
    dma = pltpu.SemaphoreType.DMA
    vmem = pltpu.VMEM
    far = pl.BlockSpec(memory_space=pltpu.HBM)
    pinned = [
        pltpu.with_memory_space_constraint(a, pltpu.HBM)
        for a in (
            inputs, gate_input, b_source, c_source, step_raw.T, step_bias[None, :],
            decay_rate[None, :], conv_weight, conv_bias[None, :],
            norm_gain.reshape(features // 128, 128), doc_lengths,
        )
    ]
    return pl.pallas_call(
        functools.partial(layer_kernel, groups, parts, heads),
        out_shape=jax.ShapeDtypeStruct((tokens, features), BF16),
        in_specs=[far] * 11,
        out_specs=pl.BlockSpec(memory_space=pltpu.VMEM),
        scratch_shapes=[
            vmem((tokens, features), BF16),
            vmem((tokens, features), BF16),
            vmem((tokens, state), BF16),
            vmem((tokens, state), BF16),
            vmem((heads, tokens), F32),
            vmem((1, heads), F32),
            vmem((1, heads), F32),
            vmem(conv_weight.shape, F32),
            vmem((1, 2 * state), F32),
            vmem((features // 128, 128), F32),
            pltpu.SMEM(doc_lengths.shape, jnp.int32),
            vmem((128, tokens), F32),
            vmem((8 + tokens, 2 * state), F32),
            vmem((2, 16, state), BF16),
            vmem((tokens, features), BF16),
            vmem((tokens, state), BF16),
            vmem((heads, tokens), F32),
            vmem((1, 128), F32),
            vmem((state, features), F32),
            vmem((SUPER, rows, lanes), F32),
            vmem((SUPER, 1, 128), F32),
            vmem((SUPER, lanes), F32),
            vmem((1, 128), F32),
            vmem((1, 128), F32),
            vmem((rows, lanes), F32),
            vmem((rows, lanes), F32),
            vmem((rows, lanes), F32),
            vmem((rows, lanes), F32),
            vmem((SUPER, rows, lanes), BF16),
            vmem((SUPER, rows, lanes), BF16),
            vmem((state, features), BF16),
            vmem((tokens, features), F32),
            vmem((tokens, features), F32),
            vmem((1, tokens), F32),
            vmem((parts - 1, 1, tokens), F32),
            dma((11,)), dma((2,)), dma((2,)), dma, dma, dma, dma,
            dma((3,)), dma((3,)),
            dma, dma, dma((parts - 1,)), dma((parts - 1,)),
            pltpu.SemaphoreType.REGULAR,
        ],
        compiler_params=pltpu.CompilerParams(
            collective_id=0, has_side_effects=True, vmem_limit_bytes=48 * 1024 * 1024
        ),
    )(*pinned)


def solution(mesh):
    both, seq = P("seq", "tp"), P("seq", None)
    return jax.shard_map(
        body, mesh=mesh,
        in_specs=(both, both, seq, seq, both, P("tp"), P("tp"), P(), P(), P("tp"), P()),
        out_specs=both, check_vma=False,
    )
```

```python
import functools

import jax
import jax.numpy as jnp
from jax import lax
from jax.experimental import pallas as pl
from jax.experimental.pallas import tpu as pltpu
from jax.sharding import PartitionSpec as P

MESH = pl.DeviceIdType.MESH
EPS = 1e-05
SUPER = 32
CODES = 32767.0
F32 = jnp.float32
BF16 = jnp.bfloat16
EXACT = lax.Precision.HIGHEST


def remote(source, target, send, recv, **device):
    return pltpu.make_async_remote_copy(
        source, target, send, recv, device_id=device, device_id_type=MESH
    )


def layer_kernel(
    groups, parts, heads,
    x_hbm, gate_hbm, b_hbm, c_hbm, step_hbm, bias_hbm, rate_hbm, taps_hbm, shift_hbm, gain_hbm,
    docs_hbm, out_ref,
    x, gate, b_ref, c_ref, step_ref, bias_ref, rate_ref, taps_ref, shift_ref, gain_ref, docs_ref,
    turned, ext, halo, weighted, c_conv, rows_c, factor, codes, grains, codes_in,
    grains_in, er, fr, wide,
    z_factor, z_factor_in, z_total, z_total_in, z_state, z_state_in, qs, qr, q, dg, rs, sums, others,
    in_sem, h_send, h_recv, f_send, f_recv, e_send, e_recv, g_send, g_recv, z_send, z_recv,
    q_send, q_recv, s_send, s_recv, ready, here,
):
    me, part = lax.axis_index("seq"), lax.axis_index("tp")
    shards = groups * SUPER
    group, place = me // SUPER, me % SUPER
    dz, dy, dx = place // 16, (place // 4) % 4, place % 4
    tokens, features = x.shape
    state = b_ref.shape[1]
    rows, lanes = er.shape[1], er.shape[2]
    width = features // heads
    pairs = features // 128

    def partner(d):
        to = ((dz + d // 16) % 2) * 16 + ((dy + (d // 4) % 4) % 4) * 4 + (dx + d % 4) % 4
        return to, group * SUPER + to

    def hops(d):
        along_y, along_x = (d // 4) % 4, d % 4
        return d // 16 + min(along_y, 4 - along_y) + min(along_x, 4 - along_x)

    farthest_first = sorted(range(1, SUPER), key=lambda d: (-hops(d), d % 4, d))

    def each(f):
        for d in farthest_first:
            f(d)

    barrier = pltpu.get_barrier_semaphore()

    def signal(**device):
        pl.semaphore_signal(barrier, 1, device_id=device, device_id_type=MESH)

    has_next, has_last = group + 1 < groups, group > 0
    has_second = group + 2 < groups
    ends_group, opens_group = place == SUPER - 1, place == 0
    pl.when(has_last)(lambda: signal(seq=me - SUPER))
    pl.when(has_last & opens_group)(lambda: signal(seq=me - 1))
    each(lambda d: signal(seq=partner(d)[1]))
    pl.when(has_next)(lambda: signal(seq=me + SUPER))
    pl.when(has_next & ends_group)(lambda: signal(seq=me + 1))
    chip_mate = part // 2 * 2 + 1 - part % 2
    signal(tp=chip_mate)
    upper = part // 2

    @pl.when(upper == 0)
    def _():
        for core in range(2):
            signal(tp=2 + core)


    def fetch(k, source, target):
        copy = pltpu.make_async_copy(source, target, in_sem.at[k])
        copy.start()
        return copy

    b_in = fetch(4, b_hbm, b_ref)
    c_in = fetch(5, c_hbm, c_ref)
    step_in = fetch(0, step_hbm, step_ref)
    bias_in = fetch(1, bias_hbm, bias_ref)
    rate_in = fetch(2, rate_hbm, rate_ref)
    docs_in = fetch(3, docs_hbm, docs_ref)
    x_in = fetch(6, x_hbm, x)
    taps_in = fetch(7, taps_hbm, taps_ref)
    shift_in = fetch(8, shift_hbm, shift_ref)
    gate_in = fetch(9, gate_hbm, gate)
    gain_in = fetch(10, gain_hbm, gain_ref)

    count = (
        SUPER - 1 + 1 + 2 * upper + has_next.astype(jnp.int32) + has_last.astype(jnp.int32)
        + (has_next & ends_group).astype(jnp.int32) + (has_last & opens_group).astype(jnp.int32)
    )
    pl.semaphore_wait(barrier, count)
    @pl.when(upper == 1)
    def _():
        for core in range(2):
            pl.semaphore_signal(here, 1, device_id={"tp": core}, device_id_type=MESH)

    @pl.when(has_last & has_next)
    def _():
        pl.semaphore_signal(ready, 1, device_id={"seq": me - SUPER}, device_id_type=MESH)

    b_in.wait()
    c_in.wait()

    def halo_copies():
        return [
            remote(
                ref.at[pl.ds(tokens - 16, 16), :], halo.at[k], h_send.at[k], h_recv.at[k],
                seq=me + 1,
            )
            for k, ref in enumerate((b_ref, c_ref))
        ]

    @pl.when(me + 1 < shards)
    def _():
        for copy in halo_copies():
            copy.start()

    docs_in.wait()
    first = me * tokens
    starts, at = [], jnp.int32(0)
    for k in range(docs_ref.shape[0]):
        starts.append(at)
        at = at + docs_ref[k]

    def locate(position):
        found = jnp.zeros_like(position)
        for start in starts:
            found = jnp.maximum(found, jnp.where(position >= start, start, 0))
        return found

    position = first + lax.broadcasted_iota(jnp.int32, (tokens, 128), 0)
    doc = locate(position)
    doc_row = locate(first + lax.broadcasted_iota(jnp.int32, (8, tokens), 1))
    doc_last = doc_row[0:1, tokens - 1 : tokens]

    step_in.wait()
    bias_in.wait()
    rate_in.wait()
    same = lax.broadcasted_iota(jnp.int32, (heads, heads), 0) == lax.broadcasted_iota(
        jnp.int32, (heads, heads), 1
    )

    def upright(row):
        return jnp.sum(jnp.where(same, jnp.broadcast_to(row, (heads, heads)), 0.0), 1, keepdims=True)

    step = jax.nn.softplus(step_ref[...] + upright(bias_ref[...]))
    log_decay = -step * upright(rate_ref[...])
    order = lax.broadcasted_iota(jnp.int32, (tokens, tokens), 0)
    across = lax.broadcasted_iota(jnp.int32, (tokens, tokens), 1)
    lower = across <= order
    cumulated = jnp.dot(
        log_decay, (order <= across).astype(F32), precision=EXACT, preferred_element_type=F32
    )
    grown = jnp.exp(cumulated)
    shrunk = jnp.exp(-cumulated) * step
    rows_c[...] = shrunk
    turned[...] = jnp.zeros_like(turned)
    turned[:heads, :] = grown
    grown_c = turned[...].T
    opened_c = jnp.where(doc < first, grown_c, 0.0)
    factor[...] = opened_c[tokens - 1 : tokens, :]
    turned[:heads, :] = jnp.where(
        doc_row[0:1, :] == doc_last, shrunk * grown[:, tokens - 1 : tokens], 0.0
    )
    weights_c = turned[...].T

    def f_copy(d):
        return remote(factor, fr.at[place], f_send, f_recv, seq=partner(d)[1])

    def e_copy(d):
        to, there = partner(d)
        return remote(codes.at[to], codes_in.at[place], e_send, e_recv, seq=there)

    def g_copy(d):
        to, there = partner(d)
        return remote(grains.at[to], grains_in.at[place], g_send, g_recv, seq=there)

    def q_copy(d):
        to, there = partner(d)
        return remote(qs.at[to], qr.at[place], q_send, q_recv, seq=there)

    def wait_all(buffer, *sems):
        part_of = buffer.at[pl.ds(0, SUPER - 1)]
        for sem in sems:
            pltpu.make_async_copy(part_of, part_of, sem).wait()

    each(lambda d: f_copy(d).start())

    low = lax.broadcasted_iota(jnp.int32, (tokens, 128), 1) < width

    def spread(columns, pair):
        one = jnp.broadcast_to(columns[:, 2 * pair : 2 * pair + 1], (tokens, 128))
        two = jnp.broadcast_to(columns[:, 2 * pair + 1 : 2 * pair + 2], (tokens, 128))
        return jnp.where(low, one, two)

    x_in.wait()
    for pair in range(pairs):
        cut = slice(128 * pair, 128 * pair + 128)
        weighted[:, cut] = (x[:, cut].astype(F32) * spread(weights_c, pair)).astype(BF16)

    taps_in.wait()
    shift_in.wait()
    ext[8:, :state] = b_ref[...].astype(F32)
    ext[8:, state:] = c_ref[...].astype(F32)

    @pl.when(me > 0)
    def _():
        for copy in halo_copies():
            copy.wait_recv()

    @pl.when(me == 0)
    def _():
        halo[...] = jnp.zeros_like(halo)

    ext[:8, :state] = halo[0].astype(F32)[8:]
    ext[:8, state:] = halo[1].astype(F32)[8:]

    def convolve(half):
        cut = slice(half * state, half * state + state)
        total = jnp.broadcast_to(shift_ref[:, cut], (tokens, state))
        for k in range(4):
            back = 3 - k
            term = taps_ref[k : k + 1, cut] * ext[8 - back : 8 - back + tokens, cut]
            total = total + jnp.where(position - back >= doc, term, 0.0)
        return total * jax.nn.sigmoid(total)

    b_turned = convolve(0).T.astype(BF16)
    slices = SUPER // 2
    for other in (1, 0):
        side = (dz + other) % 2
        ends = jnp.dot(
            b_turned, weighted[:, pl.ds(pl.multiple_of(side * lanes, 128), lanes)],
            preferred_element_type=F32,
        ).reshape(slices, rows, lanes)
        largest = jnp.maximum(jnp.max(jnp.abs(ends), 1, keepdims=True), 1e-30)
        codes[pl.ds(side * slices, slices)] = (
            jnp.round(ends * (CODES / largest)).astype(jnp.int32).astype(jnp.int16)
        )
        grains[pl.ds(side * slices, slices)] = largest * (1.0 / CODES)
        for d in farthest_first:
            if d // 16 == other:
                e_copy(d).start()
                g_copy(d).start()
    fr[place] = factor[...]
    codes_in[place] = codes[place]
    grains_in[place] = grains[place]

    c_conv[...] = convolve(1).astype(BF16)
    products = jnp.dot(c_conv[...], b_turned, preferred_element_type=F32)
    doc_wide = jnp.concatenate([doc, doc], 1)
    products = jnp.where(lower & (doc_row[0:1, :] == doc_wide), products, 0.0)
    half = tokens // 2
    top, bottom = products[:half, :half], products[half:, :]
    gate_in.wait()
    for pair in range(pairs):
        cut = slice(128 * pair, 128 * pair + 128)
        found = []
        for h in (2 * pair, 2 * pair + 1):
            decay = jnp.broadcast_to(grown_c[:, h : h + 1], (tokens, 128))
            row = rows_c[h : h + 1, :]
            low_scores = top * row[:, :half] * decay[:half]
            high = jnp.concatenate([decay[half:], decay[half:]], 1)
            high_scores = bottom * row * high
            found.append(
                jnp.concatenate(
                    [
                        jnp.dot(
                            low_scores.astype(BF16), x[:half, cut], preferred_element_type=F32
                        ),
                        jnp.dot(
                            high_scores.astype(BF16), x[:, cut], preferred_element_type=F32
                        ),
                    ],
                    0,
                )
            )
        opening = gate[:, cut].astype(F32)
        opening = opening * jax.nn.sigmoid(opening)
        dg[:, cut] = jnp.where(low, found[0], found[1]) * opening
        rs[:, cut] = spread(opened_c, pair) * opening

    wait_all(fr, f_send, f_recv)
    column = lax.broadcasted_iota(jnp.int32, (128, lanes), 1) // width
    column = column + (place // 16) * (lanes // width)
    pick = (column == lax.broadcasted_iota(jnp.int32, (128, lanes), 0)).astype(F32)
    gathered = jnp.concatenate([fr[k] for k in range(SUPER)], 0)
    wide[...] = jnp.dot(gathered, pick, precision=EXACT, preferred_element_type=F32)

    product = fr[0]
    for k in range(1, SUPER):
        product = product * fr[k]
    z_factor[...] = product

    def factor_copy():
        return remote(z_factor, z_factor_in, z_send.at[0], z_recv.at[0], seq=me + SUPER)

    def total_copy():
        return remote(z_total, z_total_in, z_send.at[1], z_recv.at[1], seq=me + SUPER)

    def state_copy():
        return remote(z_state, z_state_in, z_send.at[2], z_recv.at[2], seq=me + 2 * SUPER)

    pl.when(has_next)(lambda: factor_copy().start())

    def expand(row):
        return jnp.dot(
            jnp.broadcast_to(row, (rows, 128)), pick, precision=EXACT, preferred_element_type=F32
        )

    scale = expand(product)
    wait_all(codes_in, e_send, e_recv)
    wait_all(grains_in, g_send, g_recv)
    er[...] = codes_in[...].astype(jnp.int32).astype(F32) * grains_in[...]

    def factor_of(k):
        return jnp.broadcast_to(wide[k : k + 1, :], (rows, lanes))

    total = er[0]
    for k in range(1, SUPER):
        total = factor_of(k) * total + er[k]
    z_total[...] = total
    pl.when(has_next)(lambda: total_copy().start())

    @pl.when(group < 2)
    def _():
        z_state_in[...] = jnp.zeros_like(z_state_in)

    @pl.when(group == 0)
    def _():
        z_factor_in[...] = jnp.zeros_like(z_factor_in)
        z_total_in[...] = jnp.zeros_like(z_total_in)

    @pl.when(has_last)
    def _():
        factor_copy().wait_recv()
        total_copy().wait_recv()

    scale_in = expand(z_factor_in[...])

    @pl.when(group > 1)
    def _():
        state_copy().wait_recv()

    current = scale_in * z_state_in[...] + z_total_in[...]
    z_state[...] = scale * current + total

    @pl.when(has_second)
    def _():
        pl.semaphore_wait(ready, 1)
        state_copy().start()

    for k in range(SUPER):
        qs[k] = current.astype(BF16)
        if k + 1 < SUPER:
            current = factor_of(k) * current + er[k]
    each(lambda d: q_copy(d).start())
    qr[place] = qs[place]

    wait_all(qr, q_send, q_recv)
    for side in range(2):
        for k in range(0, 16, 2):
            both = [qr[side * 16 + k + u].astype(F32) for u in range(2)]
            q[k * rows : (k + 2) * rows, side * lanes : (side + 1) * lanes] = jnp.concatenate(
                both, 0
            ).astype(BF16)

    squares = jnp.zeros((tokens, 128), F32)
    for pair in range(pairs):
        cut = slice(128 * pair, 128 * pair + 128)
        from_state = jnp.dot(c_conv[...], q[:, cut], preferred_element_type=F32)
        gated = dg[:, cut] + from_state * rs[:, cut]
        dg[:, cut] = gated
        squares = squares + gated * gated
    sums[...] = jnp.sum(squares.T, axis=0, keepdims=True)
    copies = [
        remote(sums, others.at[k - 1], s_send.at[k - 1], s_recv.at[k - 1], tp=(part + k) % parts)
        for k in range(1, parts)
    ]
    @pl.when(upper == 0)
    def _():
        pl.semaphore_wait(here, 2)

    for copy in copies:
        copy.start()

    @pl.when(me + 1 < shards)
    def _():
        for copy in halo_copies():
            copy.wait_send()

    @pl.when(has_next)
    def _():
        factor_copy().wait_send()
        total_copy().wait_send()

    pl.when(has_second)(lambda: state_copy().wait_send())
    for copy in copies:
        copy.wait()
    mean_square = (sums[...] + others[0] + others[1] + others[2]) * (1.0 / (features * parts))
    inverse = lax.rsqrt(mean_square + EPS)
    inverse = jnp.broadcast_to(inverse, (128, tokens)).T
    gain_in.wait()
    for pair in range(pairs):
        cut = slice(128 * pair, 128 * pair + 128)
        out_ref[:, cut] = (dg[:, cut] * inverse * gain_ref[pair : pair + 1, :]).astype(BF16)


def body(
    inputs, gate_input, b_source, c_source, step_raw, step_bias, decay_rate,
    conv_weight, conv_bias, norm_gain, doc_lengths,
):
    groups, parts = lax.axis_size("seq") // SUPER, lax.axis_size("tp")
    tokens, features = inputs.shape
    heads, state = step_raw.shape[1], b_source.shape[1]
    rows, lanes = state // 16, features // 2
    dma = pltpu.SemaphoreType.DMA
    vmem = pltpu.VMEM
    far = pl.BlockSpec(memory_space=pltpu.HBM)
    pinned = [
        pltpu.with_memory_space_constraint(a, pltpu.HBM)
        for a in (
            inputs, gate_input, b_source, c_source, step_raw.T, step_bias[None, :],
            decay_rate[None, :], conv_weight, conv_bias[None, :],
            norm_gain.reshape(features // 128, 128), doc_lengths,
        )
    ]
    return pl.pallas_call(
        functools.partial(layer_kernel, groups, parts, heads),
        out_shape=jax.ShapeDtypeStruct((tokens, features), BF16),
        in_specs=[far] * 11,
        out_specs=pl.BlockSpec(memory_space=pltpu.VMEM),
        scratch_shapes=[
            vmem((tokens, features), BF16),
            vmem((tokens, features), BF16),
            vmem((tokens, state), BF16),
            vmem((tokens, state), BF16),
            vmem((heads, tokens), F32),
            vmem((1, heads), F32),
            vmem((1, heads), F32),
            vmem(conv_weight.shape, F32),
            vmem((1, 2 * state), F32),
            vmem((features // 128, 128), F32),
            pltpu.SMEM(doc_lengths.shape, jnp.int32),
            vmem((128, tokens), F32),
            vmem((8 + tokens, 2 * state), F32),
            vmem((2, 16, state), BF16),
            vmem((tokens, features), BF16),
            vmem((tokens, state), BF16),
            vmem((heads, tokens), F32),
            vmem((1, 128), F32),
            vmem((SUPER, rows, lanes), jnp.int16),
            vmem((SUPER, 1, lanes), F32),
            vmem((SUPER, rows, lanes), jnp.int16),
            vmem((SUPER, 1, lanes), F32),
            vmem((SUPER, rows, lanes), F32),
            vmem((SUPER, 1, 128), F32),
            vmem((SUPER, lanes), F32),
            vmem((1, 128), F32),
            vmem((1, 128), F32),
            vmem((rows, lanes), F32),
            vmem((rows, lanes), F32),
            vmem((rows, lanes), F32),
            vmem((rows, lanes), F32),
            vmem((SUPER, rows, lanes), BF16),
            vmem((SUPER, rows, lanes), BF16),
            vmem((state, features), BF16),
            vmem((tokens, features), F32),
            vmem((tokens, features), F32),
            vmem((1, tokens), F32),
            vmem((parts - 1, 1, tokens), F32),
            dma((11,)), dma((2,)), dma((2,)), dma, dma, dma, dma, dma, dma,
            dma((3,)), dma((3,)),
            dma, dma, dma((parts - 1,)), dma((parts - 1,)),
            pltpu.SemaphoreType.REGULAR, pltpu.SemaphoreType.REGULAR,
        ],
        compiler_params=pltpu.CompilerParams(
            collective_id=0, has_side_effects=True, vmem_limit_bytes=48 * 1024 * 1024
        ),
    )(*pinned)


def solution(mesh):
    both, seq = P("seq", "tp"), P("seq", None)
    return jax.shard_map(
        body, mesh=mesh,
        in_specs=(both, both, seq, seq, both, P("tp"), P("tp"), P(), P(), P("tp"), P()),
        out_specs=both, check_vma=False,
    )
```
